128 devices in a mesh: gene: 8 (over x, core), site: 16 (over z, y).
Axes of the slice: x: 4, y: 4, z: 4, core: 2. Of those that a mesh axis runs over, the one named last changes fastest.
Arguments:
- tips: bfloat16 [8, 32, 20, 32768], P('gene', None, None, 'site'), may hold values from 0.0009994507 to 1
- exchange: float32 [20, 20], replicated, may hold values from 0.05 to 5
- freqs: float32 [20], replicated, may hold values from 0.02 to 0.12
- rates: float32 [4], replicated, may hold values from 0.1 to 3
- branch: float32 [62], replicated, may hold values from 0.02 to 0.6
- children: int32 [31, 2], replicated, may hold values from 0 to 61, as said below
- slot_gene: int32 [8, 256], P('gene', 'site'), may hold values from 0 to 63, as said below
- site_count: int32 [8, 256], P('gene', 'site'), may hold values from 0 to 128, as said below
Outputs:
- site_loglik: float32 [8, 32768], P('gene', 'site')
- gene_loglik: float32 [8, 64], P('gene')
- total: float32 [], replicated
The draws below stay inside these ranges and needn't reach their ends.
Inputs may be any that keep to these rules, and one draw needn't show every extreme that they name: `children`: internal nodes come in 5 levels: the first 16 pair up all leaves, each next level pairs up all nodes of the level before, in node order; each node is a child once. On each device along site the slots with site_count > 0 come first; each device holds at least (64 + 16 - 1) // 16 of them and in each group one device has all 16 live; a live slot's live sites are its first ones. `slot_gene`: every gene of a group owns at least one live slot; on slots that are not live the value is 0.
All inputs are finite; a program needn't handle non-finite values.
Results may differ from the reference program's by a relative error of at most 0.0003.
Values may be sent and summed in bfloat16 or wider, within the bound.
A program may use at most 128 MiB of HBM per device.

```python
import math
import jax
import jax.numpy as jnp
from jax import lax

STATES = 20
RATES = 4
LEVELS = 5
TILE = 128
SLOTS_DEV = 16
GROUP_GENES = 64
TAXA = 32
NODES = 62
SLOTS = 256
SITES = 32768
N_GENE = 8
N_SITE = 16


def slot_layout(key):
    keys = jax.random.split(jax.random.fold_in(key, 7), 6)
    draws = jax.random.randint(keys[0], (N_GENE, N_SITE), 0, SLOTS_DEV + 1)
    lowest = (GROUP_GENES + N_SITE - 1) // N_SITE
    live = jnp.maximum(lowest, draws * draws // SLOTS_DEV)
    fullest = jax.random.randint(keys[1], (N_GENE,), 0, N_SITE)
    live = jnp.where(jnp.arange(N_SITE)[None, :] == fullest[:, None], SLOTS_DEV, live)
    alive = (jnp.arange(SLOTS_DEV)[None, None, :] < live[:, :, None]).reshape(N_GENE, SLOTS)
    index = jnp.arange(SLOTS, dtype=jnp.int32)[None, :]
    score = jax.random.randint(keys[2], (N_GENE, SLOTS), 0, 2 ** 19) * SLOTS + index
    score = jnp.where(alive, score, 2 ** 19 * SLOTS + index)
    order = jnp.argsort(score, axis=1)
    ranked = jnp.argsort(order, axis=1).astype(jnp.int32)
    others = jax.random.randint(keys[3], (N_GENE, SLOTS), 0, GROUP_GENES)
    owner = jnp.where(alive, jnp.where(ranked < GROUP_GENES, ranked, others), 0)
    partial_value = jax.random.randint(keys[4], (N_GENE, SLOTS), 1, TILE + 1)
    pick = jax.random.randint(keys[5], (N_GENE, SLOTS), 0, 4) == 0
    sizes = jnp.where(alive, jnp.where(pick, partial_value, TILE), 0)
    return (owner.astype(jnp.int32), sizes.astype(jnp.int32))


def draw_slot_gene(key, part):
    return slot_layout(key)[0]


def draw_site_count(key, part):
    return slot_layout(key)[1]


def draw_children(key, part):
    rows = []
    prev_start = 0
    next_id = TAXA
    count = TAXA
    for level in range(LEVELS):
        order = jax.random.permutation(jax.random.fold_in(key, 100 + level), count) + prev_start
        rows.append(order.reshape(count // 2, 2))
        prev_start = next_id
        next_id = next_id + count // 2
        count = count // 2
    return jnp.concatenate(rows, axis=0).astype(jnp.int32)


def level_of(rng, shape, shards, least, top_value):
    def one(axis_at, blocks):
        heights = jax.random.uniform(jax.random.fold_in(jax.random.fold_in(rng, 6), axis_at), (blocks,), jnp.float32, least / len(shards), top_value / len(shards))
        return jnp.repeat(jnp.exp(heights), shape[axis_at] // blocks).reshape((-1,) + (1,) * (len(shape) - axis_at - 1))

    factor_of = one(*shards[0])
    for cut in shards[1:]:
        factor_of = factor_of * one(*cut)
    return factor_of


def setup_inputs(seed: int = 0) -> dict:
    key_of = jax.random.split(jax.random.key(seed), 9)
    return {
        "tips": jnp.clip(jnp.exp(math.log(1.0) - 6.9083047 * jax.random.uniform(key_of[0], (N_GENE, TAXA, STATES, SITES), jnp.float32) ** level_of(key_of[0], (N_GENE, TAXA, STATES, SITES), ((0, 8), (3, 16)), -0.2, 0.2)), 0.0009994507, 1.0).astype(jnp.bfloat16),
        "exchange": jnp.clip(jnp.exp(jax.random.uniform(key_of[1], (STATES, STATES), jnp.float32, math.log(0.05), math.log(5.0))), 0.05, 5.0),
        "freqs": jnp.clip(jnp.exp(jax.random.uniform(key_of[2], (STATES,), jnp.float32, math.log(0.02), math.log(0.12))), 0.02, 0.12),
        "rates": jnp.clip(jnp.exp(jax.random.uniform(key_of[3], (RATES,), jnp.float32, math.log(0.1), math.log(3.0))), 0.1, 3.0),
        "branch": jnp.clip(jnp.exp(jax.random.uniform(key_of[4], (NODES,), jnp.float32, math.log(0.02), math.log(0.6))), 0.02, 0.6),
        "children": draw_children(jax.random.fold_in(key_of[8], 71), 0),
        "slot_gene": draw_slot_gene(jax.random.fold_in(key_of[8], 71), 0),
        "site_count": draw_site_count(jax.random.fold_in(key_of[8], 71), 0),
    }


def transitions(exchange, freqs, rates, branch):
    eye = jnp.eye(STATES, dtype=jnp.float32)
    sym = (exchange + exchange.T) * 0.5 * (1.0 - eye)
    pi = freqs / jnp.sum(freqs)
    qmat = sym * pi[None, :]
    qmat = qmat - eye * jnp.sum(qmat, axis=1)[:, None]
    qmat = qmat / (-jnp.sum(pi * jnp.diagonal(qmat)))
    scaled = rates / jnp.mean(rates)
    times = (branch[:, None] * scaled[None, :]).reshape(-1) / 256.0
    amat = qmat[:, :, None] * times[None, None, :]
    term = amat
    power = eye[:, :, None] + amat
    for order in range(2, 9):
        term = jnp.einsum("ijb,jkb->ikb", term, amat, precision=lax.Precision.HIGHEST) / order
        power = power + term
    for step in range(8):
        power = jnp.einsum("ijb,jkb->ikb", power, power, precision=lax.Precision.HIGHEST)
    return power.transpose(2, 0, 1).reshape(NODES, RATES, STATES, STATES), pi


def prune(leaves, children, pmat, pi):
    width = leaves.shape[-1]
    level_x = leaves
    level_scale = jnp.zeros((TAXA, width), jnp.float32)
    prev_start = 0
    row_start = 0
    count = TAXA
    for level in range(LEVELS):
        half = count // 2
        pairs = children[row_start:row_start + half]
        left_id = pairs[:, 0]
        right_id = pairs[:, 1]
        left_x = jnp.take(level_x, left_id - prev_start, axis=0)
        right_x = jnp.take(level_x, right_id - prev_start, axis=0)
        left_p = jnp.take(pmat, left_id, axis=0)
        right_p = jnp.take(pmat, right_id, axis=0)
        if level == 0:
            left_y = jnp.einsum("nkij,njs->nkis", left_p, left_x, precision=lax.Precision.HIGHEST)
            right_y = jnp.einsum("nkij,njs->nkis", right_p, right_x, precision=lax.Precision.HIGHEST)
        else:
            left_y = jnp.einsum("nkij,nkjs->nkis", left_p, left_x, precision=lax.Precision.HIGHEST)
            right_y = jnp.einsum("nkij,nkjs->nkis", right_p, right_x, precision=lax.Precision.HIGHEST)
        product = left_y * right_y
        top = jnp.max(product, axis=(1, 2))
        level_x = product / top[:, None, None]
        level_scale = jnp.log(top) + jnp.take(level_scale, left_id - prev_start, axis=0) + jnp.take(level_scale, right_id - prev_start, axis=0)
        prev_start = TAXA + row_start
        row_start = row_start + half
        count = half
    lik = jnp.sum(level_x[0] * pi[None, :, None], axis=(0, 1)) / RATES
    return jnp.log(lik) + level_scale[0]


def reference(tips, exchange, freqs, rates, branch, children, slot_gene, site_count):
    pmat, pi = transitions(exchange, freqs, rates, branch)
    block = 4 * TILE
    per_group = SITES // block
    zero = jnp.zeros((), jnp.int32)

    def one_block(index):
        group = (index // per_group).astype(jnp.int32)
        start = ((index % per_group) * block).astype(jnp.int32)
        piece = lax.dynamic_slice(tips, (group, zero, zero, start), (1, TAXA, STATES, block))[0]
        return prune(piece.astype(jnp.float32), children, pmat, pi)

    values = lax.map(one_block, jnp.arange(N_GENE * per_group, dtype=jnp.int32))
    values = values.reshape(N_GENE, SLOTS, TILE)
    inside = jnp.arange(TILE, dtype=jnp.int32)[None, None, :] < site_count[:, :, None]
    values = jnp.where(inside, values, 0.0)
    site_loglik = values.reshape(N_GENE, SITES)
    per_slot = jnp.sum(values, axis=2)
    genes = jnp.arange(GROUP_GENES, dtype=jnp.int32)
    hit = ((slot_gene[:, None, :] == genes[None, :, None]) & (site_count[:, None, :] > 0)).astype(jnp.float32)
    sums = jnp.sum(hit * per_slot[:, None, :], axis=2)
    counts = jnp.sum(hit * site_count.astype(jnp.float32)[:, None, :], axis=2)
    gene_loglik = sums / counts
    total = jnp.sum(per_slot) / (TILE * SLOTS)
    return site_loglik, gene_loglik, total
```

```python
import functools

import jax
import jax.numpy as jnp
from jax import lax
from jax.experimental import pallas as pl
from jax.experimental.pallas import tpu as pltpu
from jax.sharding import PartitionSpec as P

STATES = 20
RATES = 4
ROWS = STATES * RATES
LEAVES = 32
INNER = 30
NODES = 62
GENES = 64
PAD = 24
LANES = 128
SPLIT = 32
BLOCK = 512
F32 = jnp.float32
BF16 = jnp.bfloat16


def iota(shape, axis):
    return lax.broadcasted_iota(jnp.int32, shape, axis)


def rate_powers(exchange_ref, freqs_ref, pad_ref):
    pad_ref[...] = jnp.zeros((LANES, LANES), F32)
    pad_ref[0:STATES, 0:STATES] = exchange_ref[...]
    full = pad_ref[...]
    both = (full + full.T)[0:PAD, :]
    shape = (PAD, LANES)
    sub, lane = iota(shape, 0), iota(shape, 1)
    pi_sub = jnp.zeros(shape, F32)
    pi_lane = jnp.zeros(shape, F32)
    for state in range(STATES):
        value = freqs_ref[state]
        pi_sub = jnp.where(sub == state, value, pi_sub)
        pi_lane = jnp.where(lane == state, value, pi_lane)
    total = jnp.sum(pi_sub, axis=0, keepdims=True)
    pi_sub = pi_sub / total
    pi_lane = pi_lane / total
    off = jnp.where(sub == lane, 0.0, both * 0.5 * pi_sub)
    out_rate = jnp.sum(off, axis=0, keepdims=True)
    mean_rate = jnp.sum(out_rate * pi_lane[0:1], axis=1, keepdims=True)
    gen = (off - jnp.where(sub == lane, out_rate, 0.0)) / mean_rate

    def times(left, right):
        acc = left[:, 0:1] * right[0:1, :]
        for mid in range(1, STATES):
            acc = acc + left[:, mid : mid + 1] * right[mid : mid + 1, :]
        return acc

    second = times(gen, gen) * 0.5
    third = times(second, gen) * (1.0 / 3.0)
    fourth = times(second, second) * (4.0 / 24.0)
    powers = [gen, second, third, fourth]
    for order, part in ((5, gen), (6, second), (7, third), (8, fourth)):
        ratio = {5: 24.0 / 120.0, 6: 48.0 / 720.0, 7: 144.0 / 5040.0, 8: 576.0 / 40320.0}[order]
        powers.append(times(fourth, part) * ratio)
    return powers, pi_sub


def transitions(powers, rates_ref, branch_ref, mat_ref):
    shape = (1, LANES)
    lane = iota(shape, 1)
    category = lane // SPLIT
    rate = jnp.zeros(shape, F32)
    mean = jnp.zeros(shape, F32)
    for k in range(RATES):
        rate = jnp.where(category == k, rates_ref[k], rate)
        mean = mean + rates_ref[k]
    rate = rate / (mean / RATES)
    taus = []
    for half in range(2):
        length = jnp.zeros(shape, F32)
        for at in range(min(SPLIT, NODES - half * SPLIT)):
            length = jnp.where(lane % SPLIT == at, branch_ref[half * SPLIT + at], length)
        taus.append(length * rate / 256.0)
    sub = iota((PAD, LANES), 0)
    for i in range(STATES):
        columns = [jnp.broadcast_to(p[:, i : i + 1], (PAD, LANES)) for p in powers]
        eye = jnp.where(sub == i, 1.0, 0.0)
        for half in range(2):
            acc = columns[7]
            for order in range(6, -1, -1):
                acc = columns[order] + acc * taus[half]
            mat_ref[0, half, i * PAD : (i + 1) * PAD, :] = eye + acc * taus[half]

    def square(step, carry):
        src = lax.rem(step, 2)
        dst = 1 - src
        for half in range(2):
            for first in range(0, STATES, 4):
                accs = [None] * 4
                for mid in range(STATES):
                    row = mat_ref[src, half, mid * PAD : (mid + 1) * PAD, :]
                    for at in range(4):
                        where = (first + at) * PAD + mid
                        factor = mat_ref[src, half, where : where + 1, :]
                        term = factor * row
                        accs[at] = term if accs[at] is None else accs[at] + term
                for at in range(4):
                    start = (first + at) * PAD
                    mat_ref[dst, half, start : start + PAD, :] = accs[at]
        return carry

    lax.fori_loop(0, 8, square, 0)


def operands(children_ref, mat_ref, spread_ref, leaf_ref, inner_ref):
    for half in range(2):
        for group in range(4):
            block = mat_ref[0, half, group * 120 : group * 120 + LANES, :].T
            for at in range(5):
                i = group * 5 + at
                moved = block if at == 0 else pltpu.roll(block, LANES - PAD * at, 1)
                spread_ref[half, i * LANES : (i + 1) * LANES, :] = moved

    lane = iota((ROWS, LANES), 1)

    def parts(half, at):
        value = spread_ref[half, pl.ds(at, ROWS, stride=SPLIT), :]
        value = jnp.where(lane < STATES, value, 0.0)
        high = value.astype(BF16).astype(F32)
        return high, value - high

    for node in range(LEAVES // 2):
        high, low = parts(0, children_ref[0, node])
        leaf_ref[node, 0:ROWS, :] = (high + pltpu.roll(low, 32, 1)).astype(BF16)
        high, low = parts(0, children_ref[1, node])
        leaf_ref[node, ROWS : 2 * ROWS, :] = (
            pltpu.roll(high, 64, 1) + pltpu.roll(low, 96, 1)
        ).astype(BF16)

    row, col = iota((LANES, 256), 0), iota((LANES, 256), 1)
    state = lax.rem(col, ROWS) // RATES
    low_part = (col >= 2 * ROWS).astype(jnp.int32) * 32
    place = jnp.where((row == state + low_part) & (col < 3 * ROWS), 1.0, 0.0).astype(BF16)
    row, col = iota((ROWS, 256), 0), iota((ROWS, 256), 1)
    same = lax.rem(row, RATES) == lax.rem(col, RATES)
    for at in range(INNER):
        high, low = parts(1, at)
        both = (high + pltpu.roll(low, 32, 1)).astype(BF16)
        wide = jnp.dot(both, place, preferred_element_type=F32)
        inner_ref[at] = jnp.where(same, wide, 0.0).astype(BF16)


def prune_block(start, tips_ref, children_ref, leaf_ref, inner_ref, flat_ref, node_ref, weight):
    tiles = BLOCK // LANES
    for tile in range(tiles):
        lanes = pl.ds(start + tile * LANES, LANES)
        for state in range(STATES):
            rows = slice(state * LEAVES, (state + 1) * LEAVES)
            flat_ref[tile, rows, :] = tips_ref[state, :, lanes].astype(F32)

    def keep(at, value):
        high = value.astype(BF16)
        node_ref[at, 0:ROWS, :] = high
        node_ref[at, ROWS : 2 * ROWS, :] = (value - high.astype(F32)).astype(BF16)

    filler = jnp.zeros((SPLIT - PAD, BLOCK), F32)

    def leaf(at):
        rows = pl.ds(at, PAD, stride=LEAVES)
        value = jnp.concatenate([flat_ref[tile, rows, :] for tile in range(tiles)], axis=1)
        return jnp.concatenate([value, filler], axis=0).astype(BF16)

    for node in range(LEAVES // 2):
        left = leaf(children_ref[0, node])
        right = leaf(children_ref[1, node])
        stacked = jnp.concatenate([left, left, right, right], axis=0)
        both = jnp.dot(leaf_ref[node], stacked, preferred_element_type=F32)
        keep(node, both[0:ROWS] * both[ROWS:])

    def moved(child):
        high = node_ref[child, 0:ROWS, :]
        low = node_ref[child, ROWS : 2 * ROWS, :]
        stacked = jnp.concatenate([high, low, high, high[0:16]], axis=0)
        return jnp.dot(inner_ref[child], stacked, preferred_element_type=F32)

    scale = jnp.zeros((1, BLOCK), F32)
    node = LEAVES // 2
    for count in (8, 4, 2, 1):
        for _ in range(count):
            left = children_ref[0, node] - LEAVES
            right = children_ref[1, node] - LEAVES
            value = moved(left) * moved(right)
            if count == 4:
                top = jnp.max(value, axis=0, keepdims=True)
                value = value * (1.0 / top)
                scale = scale + jnp.log(top)
            if count > 1:
                keep(node, value)
            node = node + 1
    lik = jnp.sum(value * weight, axis=0, keepdims=True)
    return jnp.log(lik) + scale


def local_kernel(
    children_ref,
    gene_ref,
    count_ref,
    freqs_ref,
    rates_ref,
    branch_ref,
    exchange_ref,
    tips_hbm,
    site_ref,
    part_ref,
    tips_ref,
    pad_ref,
    mat_ref,
    spread_ref,
    leaf_ref,
    inner_ref,
    flat_ref,
    node_ref,
    weight_ref,
    sem,
):
    fetch = pltpu.make_async_copy(tips_hbm.at[0], tips_ref, sem)
    fetch.start()
    powers, pi_sub = rate_powers(exchange_ref, freqs_ref, pad_ref)
    for i in range(STATES):
        row = jnp.broadcast_to(pi_sub[i : i + 1, 0:1] / RATES, (RATES, LANES))
        weight_ref[i * RATES : (i + 1) * RATES, :] = row
    transitions(powers, rates_ref, branch_ref, mat_ref)
    operands(children_ref, mat_ref, spread_ref, leaf_ref, inner_ref)
    part_ref[...] = jnp.zeros((1, LANES), F32)
    for tile in range(BLOCK // LANES):
        empty = jnp.zeros(((PAD - STATES) * LEAVES, LANES), F32)
        flat_ref[tile, STATES * LEAVES :, :] = empty
    fetch.wait()

    def step(number, carry):
        start = pl.multiple_of(number * BLOCK, BLOCK)
        weight = weight_ref[:, 0:1]
        values = prune_block(
            start, tips_ref, children_ref, leaf_ref, inner_ref, flat_ref, node_ref, weight
        )
        lane = iota((1, LANES), 1)
        for at in range(BLOCK // LANES):
            slot = number * (BLOCK // LANES) + at
            live = count_ref[0, slot]
            gene = gene_ref[0, slot]
            part = values[:, at * LANES : (at + 1) * LANES]
            part = jnp.where(lane < live, part, 0.0)
            site_ref[:, pl.ds(start + at * LANES, LANES)] = part
            summed = jnp.sum(part, axis=1, keepdims=True)
            add = jnp.where(lane == gene, summed, 0.0)
            add = add + jnp.where(lane == gene + GENES, live.astype(F32), 0.0)
            part_ref[...] = part_ref[...] + add
        return carry

    lax.fori_loop(0, site_ref.shape[1] // BLOCK, step, 0)


def local_part(tips, exchange, freqs, rates, branch, children, slot_gene, site_count):
    sites = tips.shape[3]
    smem = pl.BlockSpec(memory_space=pltpu.SMEM)
    vmem = pl.BlockSpec(memory_space=pltpu.VMEM)
    return pl.pallas_call(
        local_kernel,
        name="local_part",
        out_shape=(
            jax.ShapeDtypeStruct((1, sites), F32),
            jax.ShapeDtypeStruct((1, LANES), F32),
        ),
        in_specs=[smem] * 6 + [vmem, pl.BlockSpec(memory_space=pl.ANY)],
        out_specs=(vmem, vmem),
        scratch_shapes=[
            pltpu.VMEM((STATES, LEAVES, sites), BF16),
            pltpu.VMEM((LANES, LANES), F32),
            pltpu.VMEM((2, 2, 512, LANES), F32),
            pltpu.VMEM((2, STATES * LANES, LANES), F32),
            pltpu.VMEM((LEAVES // 2, 2 * ROWS, LANES), BF16),
            pltpu.VMEM((INNER, ROWS, 256), BF16),
            pltpu.VMEM((BLOCK // LANES, PAD * LEAVES, LANES), F32),
            pltpu.VMEM((INNER, 2 * ROWS, BLOCK), BF16),
            pltpu.VMEM((ROWS, LANES), F32),
            pltpu.SemaphoreType.DMA,
        ],
        compiler_params=pltpu.CompilerParams(vmem_limit_bytes=60 * 1024 * 1024),
    )(children.T, slot_gene, site_count, freqs, rates, branch, exchange, tips.transpose(0, 2, 1, 3))


def sum_kernel(genes, sites, scale, part_ref, gene_ref, total_ref, site_buf, gene_buf, own_ref, site_send, site_recv, gene_send, gene_recv):
    group = lax.axis_index("gene")
    member = lax.axis_index("site")
    barrier = pltpu.get_barrier_semaphore()
    for off in range(1, sites):
        pl.semaphore_signal(barrier, inc=1, device_id={"site": lax.rem(member + off, sites)})
    for off in range(1, genes):
        pl.semaphore_signal(barrier, inc=1, device_id={"gene": lax.rem(group + off, genes)})
    pl.semaphore_wait(barrier, sites + genes - 2)
    copies = []
    for off in range(1, sites):
        copies.append(
            pltpu.make_async_remote_copy(
                src_ref=part_ref,
                dst_ref=site_buf.at[member],
                send_sem=site_send.at[off],
                recv_sem=site_recv.at[off],
                device_id={"site": lax.rem(member + off, sites)},
            )
        )
    for copy in copies:
        copy.start()
    site_buf[member] = part_ref[...]
    for copy in copies:
        copy.wait()
    summed = site_buf[0]
    for at in range(1, sites):
        summed = summed + site_buf[at]
    counts = pltpu.roll(summed, GENES, 1)
    lane = iota((1, LANES), 1)
    own = jnp.sum(jnp.where(lane < GENES, summed, 0.0), axis=1, keepdims=True)
    own = jnp.broadcast_to(own, (1, LANES))
    own_ref[...] = own
    copies = []
    for off in range(1, genes):
        copies.append(
            pltpu.make_async_remote_copy(
                src_ref=own_ref,
                dst_ref=gene_buf.at[group],
                send_sem=gene_send.at[off],
                recv_sem=gene_recv.at[off],
                device_id={"gene": lax.rem(group + off, genes)},
            )
        )
    for copy in copies:
        copy.start()
    gene_buf[group] = own
    gene_ref[...] = (summed / counts)[:, 0:GENES]
    for copy in copies:
        copy.wait()
    total = gene_buf[0]
    for at in range(1, genes):
        total = total + gene_buf[at]
    total_ref[...] = total[:, 0:1] * (1.0 / scale)


def over_devices(part, genes, sites, scale):
    vmem = pl.BlockSpec(memory_space=pltpu.VMEM)
    return pl.pallas_call(
        functools.partial(sum_kernel, genes, sites, scale),
        name="over_devices",
        out_shape=(
            jax.ShapeDtypeStruct((1, GENES), F32),
            jax.ShapeDtypeStruct((1, 1), F32),
        ),
        in_specs=[vmem],
        out_specs=(vmem, vmem),
        scratch_shapes=[
            pltpu.VMEM((sites, 1, LANES), F32),
            pltpu.VMEM((genes, 1, LANES), F32),
            pltpu.VMEM((1, LANES), F32),
            pltpu.SemaphoreType.DMA((sites,)),
            pltpu.SemaphoreType.DMA((sites,)),
            pltpu.SemaphoreType.DMA((genes,)),
            pltpu.SemaphoreType.DMA((genes,)),
        ],
        compiler_params=pltpu.CompilerParams(collective_id=0, has_side_effects=True),
    )(part)


def solution(mesh):
    genes, sites = mesh.shape["gene"], mesh.shape["site"]

    def on_device(tips, exchange, freqs, rates, branch, children, slot_gene, site_count):
        values, part = local_part(
            tips, exchange, freqs, rates, branch, children, slot_gene, site_count
        )
        scale = tips.shape[3] * sites
        gene_loglik, total = over_devices(part, genes, sites, scale)
        return values, gene_loglik, total.reshape(())

    pair = P("gene", "site")
    return jax.shard_map(
        on_device,
        mesh=mesh,
        in_specs=(P("gene", None, None, "site"), P(), P(), P(), P(), P(), pair, pair),
        out_specs=(pair, P("gene", None), P()),
        check_vma=False,
    )
```

```python
import functools

import jax
import jax.numpy as jnp
from jax import lax
from jax.experimental import pallas as pl
from jax.experimental.pallas import tpu as pltpu
from jax.sharding import PartitionSpec as P

STATES = 20
RATES = 4
ROWS = STATES * RATES
LEAVES = 32
INNER = 30
NODES = 62
GENES = 64
PAD = 24
LANES = 128
SPLIT = 32
BLOCK = 512
SPREAD = ROWS + 1
FLAT = PAD + 1
F32 = jnp.float32
BF16 = jnp.bfloat16


def iota(shape, axis):
    return lax.broadcasted_iota(jnp.int32, shape, axis)


def rate_powers(exchange_ref, freqs_ref, pad_ref):
    pad_ref[...] = jnp.zeros((LANES, LANES), F32)
    pad_ref[0:STATES, 0:STATES] = exchange_ref[...]
    full = pad_ref[...]
    both = (full + full.T)[0:PAD, :]
    shape = (PAD, LANES)
    sub, lane = iota(shape, 0), iota(shape, 1)
    pi_sub = jnp.zeros(shape, F32)
    pi_lane = jnp.zeros(shape, F32)
    for state in range(STATES):
        value = freqs_ref[state]
        pi_sub = jnp.where(sub == state, value, pi_sub)
        pi_lane = jnp.where(lane == state, value, pi_lane)
    total = jnp.sum(pi_sub, axis=0, keepdims=True)
    pi_sub = pi_sub / total
    pi_lane = pi_lane / total
    off = jnp.where(sub == lane, 0.0, both * 0.5 * pi_sub)
    out_rate = jnp.sum(off, axis=0, keepdims=True)
    mean_rate = jnp.sum(out_rate * pi_lane[0:1], axis=1, keepdims=True)
    gen = (off - jnp.where(sub == lane, out_rate, 0.0)) / mean_rate

    def times(left, right):
        acc = left[:, 0:1] * right[0:1, :]
        for mid in range(1, STATES):
            acc = acc + left[:, mid : mid + 1] * right[mid : mid + 1, :]
        return acc

    second = times(gen, gen) * 0.5
    third = times(second, gen) * (1.0 / 3.0)
    fourth = times(second, second) * (4.0 / 24.0)
    powers = [gen, second, third, fourth]
    for order, part in ((5, gen), (6, second), (7, third), (8, fourth)):
        ratio = {5: 24.0 / 120.0, 6: 48.0 / 720.0, 7: 144.0 / 5040.0, 8: 576.0 / 40320.0}[order]
        powers.append(times(fourth, part) * ratio)
    return powers, pi_sub


def transitions(powers, rates_ref, branch_ref, mat_ref):
    shape = (1, LANES)
    lane = iota(shape, 1)
    category = lane // SPLIT
    rate = jnp.zeros(shape, F32)
    mean = jnp.zeros(shape, F32)
    for k in range(RATES):
        rate = jnp.where(category == k, rates_ref[k], rate)
        mean = mean + rates_ref[k]
    rate = rate / (mean / RATES)
    taus = []
    for half in range(2):
        length = jnp.zeros(shape, F32)
        for at in range(min(SPLIT, NODES - half * SPLIT)):
            length = jnp.where(lane % SPLIT == at, branch_ref[half * SPLIT + at], length)
        taus.append(length * rate / 256.0)
    sub = iota((PAD, LANES), 0)
    for i in range(STATES):
        columns = [jnp.broadcast_to(p[:, i : i + 1], (PAD, LANES)) for p in powers]
        eye = jnp.where(sub == i, 1.0, 0.0)
        for half in range(2):
            acc = columns[7]
            for order in range(6, -1, -1):
                acc = columns[order] + acc * taus[half]
            mat_ref[0, half, i * PAD : (i + 1) * PAD, :] = eye + acc * taus[half]

    def square(step, carry):
        src = lax.rem(step, 2)
        dst = 1 - src
        for half in range(2):
            for first in range(0, STATES, 4):
                accs = [None] * 4
                for mid in range(STATES):
                    row = mat_ref[src, half, mid * PAD : (mid + 1) * PAD, :]
                    for at in range(4):
                        where = (first + at) * PAD + mid
                        factor = mat_ref[src, half, where : where + 1, :]
                        term = factor * row
                        accs[at] = term if accs[at] is None else accs[at] + term
                for at in range(4):
                    start = (first + at) * PAD
                    mat_ref[dst, half, start : start + PAD, :] = accs[at]
        return carry

    lax.fori_loop(0, 8, square, 0)


def operands(children_ref, mat_ref, spread_ref, leaf_ref, inner_ref):
    for half in range(2):
        for group in range(4):
            block = mat_ref[0, half, group * 120 : group * 120 + LANES, :].T
            for at in range(5):
                i = group * 5 + at
                moved = block if at == 0 else pltpu.roll(block, LANES - PAD * at, 1)
                for k in range(RATES):
                    rows = pl.ds(i * RATES + k, SPLIT, stride=SPREAD)
                    spread_ref[half, rows, :] = moved[k * SPLIT : (k + 1) * SPLIT]

    lane = iota((ROWS, LANES), 1)

    def parts(half, at):
        value = spread_ref[half, pl.ds(at * SPREAD, ROWS), :]
        value = jnp.where(lane < STATES, value, 0.0)
        high = value.astype(BF16).astype(F32)
        return high, value - high

    for node in range(LEAVES // 2):
        high, low = parts(0, children_ref[0, node])
        leaf_ref[node, 0:ROWS, :] = (high + pltpu.roll(low, 32, 1)).astype(BF16)
        high, low = parts(0, children_ref[1, node])
        leaf_ref[node, ROWS : 2 * ROWS, :] = (
            pltpu.roll(high, 64, 1) + pltpu.roll(low, 96, 1)
        ).astype(BF16)

    row, col = iota((LANES, 256), 0), iota((LANES, 256), 1)
    state = lax.rem(col, ROWS) // RATES
    low_part = (col >= 2 * ROWS).astype(jnp.int32) * 32
    place = jnp.where((row == state + low_part) & (col < 3 * ROWS), 1.0, 0.0).astype(BF16)
    row, col = iota((ROWS, 256), 0), iota((ROWS, 256), 1)
    same = lax.rem(row, RATES) == lax.rem(col, RATES)
    for at in range(INNER):
        node = LEAVES // 2 + at // 2
        child = jnp.clip(children_ref[at % 2, node] - LEAVES, 0, INNER - 1)
        high, low = parts(1, child)
        both = (high + pltpu.roll(low, 32, 1)).astype(BF16)
        wide = jnp.dot(both, place, preferred_element_type=F32)
        inner_ref[at] = jnp.where(same, wide, 0.0).astype(BF16)


def prune_block(start, tips_ref, children_ref, leaf_ref, inner_ref, flat_ref, level_refs, weight):
    tiles = BLOCK // LANES
    for tile in range(tiles):
        lanes = pl.ds(start + tile * LANES, LANES)
        for state in range(STATES):
            rows = pl.ds(state, LEAVES, stride=FLAT)
            flat_ref[tile, rows, :] = tips_ref[state, :, lanes].astype(F32)

    def keep(ref, at, value):
        high = value.astype(BF16)
        ref[at, 0:ROWS, :] = high
        ref[at, ROWS : 2 * ROWS, :] = (value - high.astype(F32)).astype(BF16)

    filler = jnp.zeros((SPLIT - PAD, BLOCK), F32)

    def leaf(at):
        rows = pl.ds(at * FLAT, PAD)
        value = jnp.concatenate([flat_ref[tile, rows, :] for tile in range(tiles)], axis=1)
        return jnp.concatenate([value, filler], axis=0).astype(BF16)

    for node in range(LEAVES // 2):
        left = leaf(children_ref[0, node])
        right = leaf(children_ref[1, node])
        stacked = jnp.concatenate([left, left, right, right], axis=0)
        both = jnp.dot(leaf_ref[node], stacked, preferred_element_type=F32)
        keep(level_refs[0], node, both[0:ROWS] * both[ROWS:])

    def moved(at, ref, child):
        high = ref[child, 0:ROWS, :]
        low = ref[child, ROWS : 2 * ROWS, :]
        stacked = jnp.concatenate([high, low, high, high[0:16]], axis=0)
        return jnp.dot(inner_ref[at], stacked, preferred_element_type=F32)

    scale = jnp.zeros((1, BLOCK), F32)
    node = LEAVES // 2
    begin = LEAVES
    for level, count in enumerate((8, 4, 2, 1)):
        ref = level_refs[level]
        for place in range(count):
            left = jnp.clip(children_ref[0, node] - begin, 0, 2 * count - 1)
            right = jnp.clip(children_ref[1, node] - begin, 0, 2 * count - 1)
            at = 2 * node - LEAVES
            value = moved(at, ref, left) * moved(at + 1, ref, right)
            if count == 4:
                top = jnp.max(value, axis=0, keepdims=True)
                value = value * (1.0 / top)
                scale = scale + jnp.log(top)
            if count > 1:
                keep(level_refs[level + 1], place, value)
            node = node + 1
        begin = begin + 2 * count
    lik = jnp.sum(value * weight, axis=0, keepdims=True)
    return jnp.log(lik) + scale


def exchange(axis, size, own_ref, buf, send, recv):
    me = lax.axis_index(axis)
    copies = []
    for off in range(1, size):
        copies.append(
            pltpu.make_async_remote_copy(
                src_ref=own_ref,
                dst_ref=buf.at[me],
                send_sem=send.at[off],
                recv_sem=recv.at[off],
                device_id={axis: lax.rem(me + off, size)},
            )
        )
    for copy in copies:
        copy.start()
    buf[me] = own_ref[...]
    return copies


def total_of(copies, buf, size):
    for copy in copies:
        copy.wait()
    summed = buf[0]
    for at in range(1, size):
        summed = summed + buf[at]
    return summed


def kernel(
    mesh_shape,
    scale,
    children_ref,
    gene_ref,
    count_ref,
    freqs_ref,
    rates_ref,
    branch_ref,
    exchange_ref,
    tips_hbm,
    site_ref,
    mean_ref,
    total_ref,
    tips_ref,
    pad_ref,
    mat_ref,
    spread_ref,
    leaf_ref,
    inner_ref,
    flat_ref,
    level_refs,
    weight_ref,
    part_ref,
    own_ref,
    site_buf,
    gene_buf,
    fetch_sem,
    site_sems,
    gene_sems,
):
    genes, sites = mesh_shape
    barrier = pltpu.get_barrier_semaphore()
    for axis, size in (("site", sites), ("gene", genes)):
        for off in range(1, size):
            peer = lax.rem(lax.axis_index(axis) + off, size)
            pl.semaphore_signal(barrier, inc=1, device_id={axis: peer})
    fetch = pltpu.make_async_copy(tips_hbm.at[0], tips_ref, fetch_sem)
    fetch.start()
    powers, pi_sub = rate_powers(exchange_ref, freqs_ref, pad_ref)
    for i in range(STATES):
        row = jnp.broadcast_to(pi_sub[i : i + 1, 0:1] / RATES, (RATES, LANES))
        weight_ref[i * RATES : (i + 1) * RATES, :] = row
    transitions(powers, rates_ref, branch_ref, mat_ref)
    operands(children_ref, mat_ref, spread_ref, leaf_ref, inner_ref)
    part_ref[...] = jnp.zeros((1, LANES), F32)
    for tile in range(BLOCK // LANES):
        flat_ref[tile] = jnp.zeros((LEAVES * FLAT, LANES), F32)
    fetch.wait()
    lane = iota((1, LANES), 1)

    def step(number, carry):
        start = pl.multiple_of(number * BLOCK, BLOCK)
        weight = weight_ref[:, 0:1]
        values = prune_block(
            start, tips_ref, children_ref, leaf_ref, inner_ref, flat_ref, level_refs, weight
        )
        for at in range(BLOCK // LANES):
            slot = number * (BLOCK // LANES) + at
            live = count_ref[0, slot]
            gene = gene_ref[0, slot]
            part = values[:, at * LANES : (at + 1) * LANES]
            part = jnp.where(lane < live, part, 0.0)
            site_ref[:, pl.ds(start + at * LANES, LANES)] = part
            summed = jnp.sum(part, axis=1, keepdims=True)
            add = jnp.where(lane == gene, summed, 0.0)
            add = add + jnp.where(lane == gene + GENES, live.astype(F32), 0.0)
            part_ref[...] = part_ref[...] + add
        return carry

    lax.fori_loop(0, site_ref.shape[1] // BLOCK, step, 0)
    pl.semaphore_wait(barrier, sites + genes - 2)
    copies = exchange("site", sites, part_ref, site_buf, site_sems.at[0], site_sems.at[1])
    summed = total_of(copies, site_buf, sites)
    own = jnp.sum(jnp.where(lane < GENES, summed, 0.0), axis=1, keepdims=True)
    own_ref[...] = jnp.broadcast_to(own, (1, LANES))
    copies = exchange("gene", genes, own_ref, gene_buf, gene_sems.at[0], gene_sems.at[1])
    mean_ref[...] = (summed / pltpu.roll(summed, GENES, 1))[:, 0:GENES]
    total_ref[...] = total_of(copies, gene_buf, genes)[:, 0:1] * (1.0 / scale)


def likelihoods(genes, width, tips, exchange_, freqs, rates, branch, children, slot_gene, site_count):
    sites = tips.shape[3]
    smem = pl.BlockSpec(memory_space=pltpu.SMEM)
    vmem = pl.BlockSpec(memory_space=pltpu.VMEM)
    return pl.pallas_call(
        functools.partial(kernel, (genes, width), sites * width),
        name="likelihoods",
        out_shape=(
            jax.ShapeDtypeStruct((1, sites), F32),
            jax.ShapeDtypeStruct((1, GENES), F32),
            jax.ShapeDtypeStruct((1, 1), F32),
        ),
        in_specs=[smem] * 6 + [vmem, pl.BlockSpec(memory_space=pl.ANY)],
        out_specs=(vmem, vmem, vmem),
        scratch_shapes=[
            pltpu.VMEM((STATES, LEAVES, sites), BF16),
            pltpu.VMEM((LANES, LANES), F32),
            pltpu.VMEM((2, 2, 512, LANES), F32),
            pltpu.VMEM((2, SPLIT * SPREAD, LANES), F32),
            pltpu.VMEM((LEAVES // 2, 2 * ROWS, LANES), BF16),
            pltpu.VMEM((INNER, ROWS, 256), BF16),
            pltpu.VMEM((BLOCK // LANES, FLAT * LEAVES, LANES), F32),
            [pltpu.VMEM((count, 2 * ROWS, BLOCK), BF16) for count in (16, 8, 4, 2)],
            pltpu.VMEM((ROWS, LANES), F32),
            pltpu.VMEM((1, LANES), F32),
            pltpu.VMEM((1, LANES), F32),
            pltpu.VMEM((width, 1, LANES), F32),
            pltpu.VMEM((genes, 1, LANES), F32),
            pltpu.SemaphoreType.DMA,
            pltpu.SemaphoreType.DMA((2, width)),
            pltpu.SemaphoreType.DMA((2, genes)),
        ],
        compiler_params=pltpu.CompilerParams(
            vmem_limit_bytes=60 * 1024 * 1024, collective_id=0, has_side_effects=True
        ),
    )(
        children.T,
        slot_gene,
        site_count,
        freqs,
        rates,
        branch,
        exchange_,
        tips.transpose(0, 2, 1, 3),
    )


def solution(mesh):
    genes, sites = mesh.shape["gene"], mesh.shape["site"]

    def on_device(*args):
        values, gene_loglik, total = likelihoods(genes, sites, *args)
        return values, gene_loglik, total.reshape(())

    pair = P("gene", "site")
    return jax.shard_map(
        on_device,
        mesh=mesh,
        in_specs=(P("gene", None, None, "site"), P(), P(), P(), P(), P(), pair, pair),
        out_specs=(pair, P("gene", None), P()),
        check_vma=False,
    )
```

```python
import functools

import jax
import jax.numpy as jnp
from jax import lax
from jax.experimental import pallas as pl
from jax.experimental.pallas import tpu as pltpu
from jax.sharding import PartitionSpec as P

STATES = 20
RATES = 4
ROWS = STATES * RATES
LEAVES = 32
INNER = 30
NODES = 62
GENES = 64
PAD = 24
LANES = 128
SPLIT = 32
CHUNK = 256
LEVEL_NODES = (16, 8, 4, 2)
SQUARINGS = 8
SPREAD = ROWS + 1
FLAT = PAD + 1
F32 = jnp.float32
BF16 = jnp.bfloat16


def iota(shape, axis):
    return lax.broadcasted_iota(jnp.int32, shape, axis)


def rate_powers(exchange_ref, freqs_ref, pad_ref):
    pad_ref[...] = jnp.zeros((LANES, LANES), F32)
    pad_ref[0:STATES, 0:STATES] = exchange_ref[...]
    full = pad_ref[...]
    both = (full + full.T)[0:PAD, :]
    shape = (PAD, LANES)
    sub, lane = iota(shape, 0), iota(shape, 1)
    pi_sub = jnp.zeros(shape, F32)
    pi_lane = jnp.zeros(shape, F32)
    for state in range(STATES):
        value = freqs_ref[state]
        pi_sub = jnp.where(sub == state, value, pi_sub)
        pi_lane = jnp.where(lane == state, value, pi_lane)
    total = jnp.sum(pi_sub, axis=0, keepdims=True)
    pi_sub = pi_sub / total
    pi_lane = pi_lane / total
    off = jnp.where(sub == lane, 0.0, both * 0.5 * pi_sub)
    out_rate = jnp.sum(off, axis=0, keepdims=True)
    mean_rate = jnp.sum(out_rate * pi_lane[0:1], axis=1, keepdims=True)
    gen = (off - jnp.where(sub == lane, out_rate, 0.0)) / mean_rate

    def times(left, right):
        acc = left[:, 0:1] * right[0:1, :]
        for mid in range(1, STATES):
            acc = acc + left[:, mid : mid + 1] * right[mid : mid + 1, :]
        return acc

    second = times(gen, gen) * 0.5
    third = times(second, gen) * (1.0 / 3.0)
    fourth = times(second, second) * (4.0 / 24.0)
    powers = [gen, second, third, fourth]
    for order, part in ((5, gen), (6, second), (7, third), (8, fourth)):
        ratio = {5: 24.0 / 120.0, 6: 48.0 / 720.0, 7: 144.0 / 5040.0, 8: 576.0 / 40320.0}[order]
        powers.append(times(fourth, part) * ratio)
    return powers, pi_sub


def taylor(powers, rates_ref, branch_ref, mat_ref):
    shape = (1, LANES)
    lane = iota(shape, 1)
    category = lane // SPLIT
    rate = jnp.zeros(shape, F32)
    mean = jnp.zeros(shape, F32)
    for k in range(RATES):
        rate = jnp.where(category == k, rates_ref[k], rate)
        mean = mean + rates_ref[k]
    rate = rate / (mean / RATES)
    taus = []
    for half in range(2):
        length = jnp.zeros(shape, F32)
        for at in range(min(SPLIT, NODES - half * SPLIT)):
            length = jnp.where(lane % SPLIT == at, branch_ref[half * SPLIT + at], length)
        taus.append(length * rate / 256.0)
    sub = iota((PAD, LANES), 0)
    for i in range(STATES):
        columns = [jnp.broadcast_to(p[:, i : i + 1], (PAD, LANES)) for p in powers]
        eye = jnp.where(sub == i, 1.0, 0.0)
        for half in range(2):
            acc = columns[7]
            for order in range(6, -1, -1):
                acc = columns[order] + acc * taus[half]
            mat_ref[0, half, i * PAD : (i + 1) * PAD, :] = eye + acc * taus[half]


def square(step, half, mat_ref, beside=None):
    src = lax.rem(step, 2)
    dst = 1 - src
    for first in range(0, STATES, 4):
        if beside is not None:
            beside(first // 4)
        accs = [None] * 4
        for mid in range(STATES):
            row = mat_ref[src, half, mid * PAD : (mid + 1) * PAD, :]
            for at in range(4):
                where = (first + at) * PAD + mid
                factor = mat_ref[src, half, where : where + 1, :]
                term = factor * row
                accs[at] = term if accs[at] is None else accs[at] + term
        for at in range(4):
            start = (first + at) * PAD
            mat_ref[dst, half, start : start + PAD, :] = accs[at]


def tree_order(children_ref, order_ref):
    place = NODES
    parents = [NODES]
    for count in (2, 4, 8, 16, 32):
        place = place - count
        ids = []
        for at, parent in enumerate(parents):
            row = jnp.clip(parent - LEAVES, 0, NODES - LEAVES)
            for side in range(2):
                child = children_ref[side, row]
                order_ref[place + 2 * at + side] = child
                ids.append(child)
        parents = ids


def spread(half, mat_ref, spread_ref):
    for group in range(4):
        block = mat_ref[0, half, group * 120 : group * 120 + LANES, :].T
        for at in range(5):
            i = group * 5 + at
            moved = block if at == 0 else pltpu.roll(block, LANES - PAD * at, 1)
            for k in range(RATES):
                rows = pl.ds(i * RATES + k, SPLIT, stride=SPREAD)
                spread_ref[half, rows, :] = moved[k * SPLIT : (k + 1) * SPLIT]


def parts(half, at, spread_ref):
    value = spread_ref[half, pl.ds(at * SPREAD, ROWS), :]
    value = jnp.where(iota((ROWS, LANES), 1) < STATES, value, 0.0)
    high = value.astype(BF16).astype(F32)
    return high, value - high


def leaf_operands(order_ref, spread_ref, leaf_ref):
    for node in range(LEAVES // 2):
        high, low = parts(0, jnp.clip(order_ref[2 * node], 0, LEAVES - 1), spread_ref)
        leaf_ref[node, 0:ROWS, :] = (high + pltpu.roll(low, 32, 1)).astype(BF16)
        high, low = parts(0, jnp.clip(order_ref[2 * node + 1], 0, LEAVES - 1), spread_ref)
        leaf_ref[node, ROWS : 2 * ROWS, :] = (
            pltpu.roll(high, 64, 1) + pltpu.roll(low, 96, 1)
        ).astype(BF16)


def inner_operands(order_ref, spread_ref, inner_ref):
    row, col = iota((LANES, 256), 0), iota((LANES, 256), 1)
    state = lax.rem(col, ROWS) // RATES
    low_part = (col >= 2 * ROWS).astype(jnp.int32) * 32
    place = jnp.where((row == state + low_part) & (col < 3 * ROWS), 1.0, 0.0).astype(BF16)
    row, col = iota((ROWS, 256), 0), iota((ROWS, 256), 1)
    same = lax.rem(row, RATES) == lax.rem(col, RATES)
    for at in range(INNER):
        child = jnp.clip(order_ref[LEAVES + at] - LEAVES, 0, INNER - 1)
        high, low = parts(1, child, spread_ref)
        both = (high + pltpu.roll(low, 32, 1)).astype(BF16)
        wide = jnp.dot(both, place, preferred_element_type=F32)
        inner_ref[at] = jnp.where(same, wide, 0.0).astype(BF16)


def gather_leaves(chunk, tips_ref, order_ref, flat_ref, leaves_ref):
    tiles = CHUNK // LANES
    for tile in range(tiles):
        lanes = pl.ds(pl.multiple_of(chunk * CHUNK, CHUNK) + tile * LANES, LANES)
        for state in range(STATES):
            rows = pl.ds(state, LEAVES, stride=FLAT)
            flat_ref[tile, rows, :] = tips_ref[state, :, lanes].astype(F32)
    filler = jnp.zeros((SPLIT - PAD, CHUNK), F32)
    for at in range(LEAVES):
        rows = pl.ds(jnp.clip(order_ref[at], 0, LEAVES - 1) * FLAT, PAD)
        value = jnp.concatenate([flat_ref[tile, rows, :] for tile in range(tiles)], axis=1)
        value = jnp.concatenate([value, filler], axis=0).astype(BF16)
        leaves_ref[chunk, at * SPLIT : (at + 1) * SPLIT, :] = value


def keep(ref, chunk, at, value):
    high = value.astype(BF16)
    ref[chunk, at, 0:ROWS, :] = high
    ref[chunk, at, ROWS : 2 * ROWS, :] = (value - high.astype(F32)).astype(BF16)


def prune_leaves(nodes, chunk, leaves_ref, leaf_ref, level_ref):
    for node in nodes:
        left = leaves_ref[chunk, 2 * node * SPLIT : (2 * node + 1) * SPLIT, :]
        right = leaves_ref[chunk, (2 * node + 1) * SPLIT : (2 * node + 2) * SPLIT, :]
        stacked = jnp.concatenate([left, left, right, right], axis=0)
        both = jnp.dot(leaf_ref[node], stacked, preferred_element_type=F32)
        keep(level_ref, chunk, node, both[0:ROWS] * both[ROWS:])


def prune_inner(chunks, inner_ref, level_refs, weight):
    def moved(at, ref, chunk, child):
        high = ref[chunk, child, 0:ROWS, :]
        low = ref[chunk, child, ROWS : 2 * ROWS, :]
        stacked = jnp.concatenate([high, low, high], axis=0)
        return jnp.dot(inner_ref[at, :, 0 : 3 * ROWS], stacked, preferred_element_type=F32)

    scales = [jnp.zeros((1, CHUNK), F32) for _ in range(chunks)]
    results = []
    base = 0
    for level, count in enumerate(LEVEL_NODES):
        ref = level_refs[level]
        parents = count // 2
        for chunk in range(chunks):
            for place in range(parents):
                at = base + 2 * place
                value = moved(at, ref, chunk, 2 * place) * moved(at + 1, ref, chunk, 2 * place + 1)
                if parents == 4:
                    top = jnp.max(value, axis=0, keepdims=True)
                    value = value * (1.0 / top)
                    scales[chunk] = scales[chunk] + jnp.log(top)
                if parents > 1:
                    keep(level_refs[level + 1], chunk, place, value)
                else:
                    lik = jnp.sum(value * weight, axis=0, keepdims=True)
                    results.append(jnp.log(lik) + scales[chunk])
        base = base + count
    return results


def exchange(axis, size, own_ref, buf, send, recv):
    me = lax.axis_index(axis)
    copies = []
    for off in range(1, size):
        copies.append(
            pltpu.make_async_remote_copy(
                src_ref=own_ref,
                dst_ref=buf.at[me],
                send_sem=send.at[off],
                recv_sem=recv.at[off],
                device_id={axis: lax.rem(me + off, size)},
            )
        )
    for copy in copies:
        copy.start()
    buf[me] = own_ref[...]
    return copies


def total_of(copies, buf, size):
    for copy in copies:
        copy.wait()
    summed = buf[0]
    for at in range(1, size):
        summed = summed + buf[at]
    return summed


def kernel(
    mesh_shape,
    scale,
    children_ref,
    gene_ref,
    count_ref,
    freqs_ref,
    rates_ref,
    branch_ref,
    exchange_ref,
    tips_hbm,
    site_ref,
    mean_ref,
    total_ref,
    tips_ref,
    order_ref,
    leaves_ref,
    pad_ref,
    mat_ref,
    spread_ref,
    leaf_ref,
    inner_ref,
    flat_ref,
    level_refs,
    weight_ref,
    part_ref,
    own_ref,
    site_buf,
    gene_buf,
    fetch_sems,
    site_sems,
    gene_sems,
):
    genes, sites = mesh_shape
    barrier = pltpu.get_barrier_semaphore()
    for axis, size in (("site", sites), ("gene", genes)):
        for off in range(1, size):
            peer = lax.rem(lax.axis_index(axis) + off, size)
            pl.semaphore_signal(barrier, inc=1, device_id={axis: peer})
    chunks = site_ref.shape[1] // CHUNK

    def fetch(chunk):
        lanes = pl.ds(pl.multiple_of(chunk * CHUNK, CHUNK), CHUNK)
        return pltpu.make_async_copy(
            tips_hbm.at[0, :, :, lanes], tips_ref.at[:, :, lanes], fetch_sems.at[chunk]
        )

    for chunk in range(chunks):
        fetch(chunk).start()
    tree_order(children_ref, order_ref)
    for tile in range(CHUNK // LANES):
        flat_ref[tile] = jnp.zeros((LEAVES * FLAT, LANES), F32)
    powers, pi_sub = rate_powers(exchange_ref, freqs_ref, pad_ref)
    for i in range(STATES):
        row = jnp.broadcast_to(pi_sub[i : i + 1, 0:1] / RATES, (RATES, LANES))
        weight_ref[i * RATES : (i + 1) * RATES, :] = row

    taylor(powers, rates_ref, branch_ref, mat_ref)
    per_step = chunks // SQUARINGS

    def leaf_branches(step, carry):
        for at in range(per_step):
            chunk = step * per_step + at
            fetch(chunk).wait()
            gather_leaves(chunk, tips_ref, order_ref, flat_ref, leaves_ref)
        square(step, 0, mat_ref)
        return carry

    lax.fori_loop(0, SQUARINGS, leaf_branches, 0)
    spread(0, mat_ref, spread_ref)
    leaf_operands(order_ref, spread_ref, leaf_ref)

    def inner_branches(step, carry):
        def beside(number):
            for at in range(per_step):
                nodes = range(LEAVES // 2 * number // 5, LEAVES // 2 * (number + 1) // 5)
                prune_leaves(nodes, step * per_step + at, leaves_ref, leaf_ref, level_refs[0])

        square(step, 1, mat_ref, beside)
        return carry

    lax.fori_loop(0, SQUARINGS, inner_branches, 0)
    spread(1, mat_ref, spread_ref)
    inner_operands(order_ref, spread_ref, inner_ref)
    results = prune_inner(chunks, inner_ref, level_refs, weight_ref[:, 0:1])
    lane = iota((1, LANES), 1)
    gathered = jnp.zeros((1, LANES), F32)
    for slot in range(chunks * CHUNK // LANES):
        live = count_ref[0, slot]
        gene = gene_ref[0, slot]
        at = slot * LANES % CHUNK
        part = results[slot * LANES // CHUNK][:, at : at + LANES]
        part = jnp.where(lane < live, part, 0.0)
        site_ref[:, slot * LANES : (slot + 1) * LANES] = part
        summed = jnp.sum(part, axis=1, keepdims=True)
        gathered = gathered + jnp.where(lane == gene, summed, 0.0)
        gathered = gathered + jnp.where(lane == gene + GENES, live.astype(F32), 0.0)
    part_ref[...] = gathered
    pl.semaphore_wait(barrier, sites + genes - 2)
    copies = exchange("site", sites, part_ref, site_buf, site_sems.at[0], site_sems.at[1])
    summed = total_of(copies, site_buf, sites)
    own = jnp.sum(jnp.where(lane < GENES, summed, 0.0), axis=1, keepdims=True)
    own_ref[...] = jnp.broadcast_to(own, (1, LANES))
    copies = exchange("gene", genes, own_ref, gene_buf, gene_sems.at[0], gene_sems.at[1])
    mean_ref[...] = (summed / pltpu.roll(summed, GENES, 1))[:, 0:GENES]
    total_ref[...] = total_of(copies, gene_buf, genes)[:, 0:1] * (1.0 / scale)


def likelihoods(genes, width, tips, exchange_, freqs, rates, branch, children, slot_gene, site_count):
    sites = tips.shape[3]
    chunks = sites // CHUNK
    smem = pl.BlockSpec(memory_space=pltpu.SMEM)
    vmem = pl.BlockSpec(memory_space=pltpu.VMEM)
    return pl.pallas_call(
        functools.partial(kernel, (genes, width), sites * width),
        name="likelihoods",
        out_shape=(
            jax.ShapeDtypeStruct((1, sites), F32),
            jax.ShapeDtypeStruct((1, GENES), F32),
            jax.ShapeDtypeStruct((1, 1), F32),
        ),
        in_specs=[smem] * 6 + [vmem, pl.BlockSpec(memory_space=pl.ANY)],
        out_specs=(vmem, vmem, vmem),
        scratch_shapes=[
            pltpu.VMEM((STATES, LEAVES, sites), BF16),
            pltpu.SMEM((NODES,), jnp.int32),
            pltpu.VMEM((chunks, LEAVES * SPLIT, CHUNK), BF16),
            pltpu.VMEM((LANES, LANES), F32),
            pltpu.VMEM((2, 2, 512, LANES), F32),
            pltpu.VMEM((2, SPLIT * SPREAD, LANES), F32),
            pltpu.VMEM((LEAVES // 2, 2 * ROWS, LANES), BF16),
            pltpu.VMEM((INNER, ROWS, 256), BF16),
            pltpu.VMEM((CHUNK // LANES, FLAT * LEAVES, LANES), F32),
            [pltpu.VMEM((chunks, count, 2 * ROWS, CHUNK), BF16) for count in LEVEL_NODES],
            pltpu.VMEM((ROWS, LANES), F32),
            pltpu.VMEM((1, LANES), F32),
            pltpu.VMEM((1, LANES), F32),
            pltpu.VMEM((width, 1, LANES), F32),
            pltpu.VMEM((genes, 1, LANES), F32),
            pltpu.SemaphoreType.DMA((chunks,)),
            pltpu.SemaphoreType.DMA((2, width)),
            pltpu.SemaphoreType.DMA((2, genes)),
        ],
        compiler_params=pltpu.CompilerParams(
            vmem_limit_bytes=60 * 1024 * 1024, collective_id=0, has_side_effects=True
        ),
    )(
        children.T,
        slot_gene,
        site_count,
        freqs,
        rates,
        branch,
        exchange_,
        tips.transpose(0, 2, 1, 3),
    )


def solution(mesh):
    genes, sites = mesh.shape["gene"], mesh.shape["site"]

    def on_device(*args):
        values, gene_loglik, total = likelihoods(genes, sites, *args)
        return values, gene_loglik, total.reshape(())

    pair = P("gene", "site")
    return jax.shard_map(
        on_device,
        mesh=mesh,
        in_specs=(P("gene", None, None, "site"), P(), P(), P(), P(), P(), pair, pair),
        out_specs=(pair, P("gene", None), P()),
        check_vma=False,
    )
```

```python
import functools

import jax
import jax.numpy as jnp
from jax import lax
from jax.experimental import pallas as pl
from jax.experimental.pallas import tpu as pltpu
from jax.sharding import PartitionSpec as P

STATES = 20
RATES = 4
ROWS = STATES * RATES
LEAVES = 32
INNER = 30
NODES = 62
GENES = 64
PAD = 24
LANES = 128
SPLIT = 32
CHUNK = 256
LEVEL_NODES = (16, 8, 4, 2)
SQUARINGS = 8
SPREAD = ROWS + 1
FLAT = PAD + 1
F32 = jnp.float32
BF16 = jnp.bfloat16


def iota(shape, axis):
    return lax.broadcasted_iota(jnp.int32, shape, axis)


def rate_powers(exchange_ref, freqs_ref, pad_ref):
    pad_ref[...] = jnp.zeros((LANES, LANES), F32)
    pad_ref[0:STATES, 0:STATES] = exchange_ref[...]
    full = pad_ref[...]
    both = (full + full.T)[0:PAD, :]
    shape = (PAD, LANES)
    sub, lane = iota(shape, 0), iota(shape, 1)
    pi_sub = jnp.zeros(shape, F32)
    pi_lane = jnp.zeros(shape, F32)
    for state in range(STATES):
        value = freqs_ref[state]
        pi_sub = jnp.where(sub == state, value, pi_sub)
        pi_lane = jnp.where(lane == state, value, pi_lane)
    total = jnp.sum(pi_sub, axis=0, keepdims=True)
    pi_sub = pi_sub / total
    pi_lane = pi_lane / total
    off = jnp.where(sub == lane, 0.0, both * 0.5 * pi_sub)
    out_rate = jnp.sum(off, axis=0, keepdims=True)
    mean_rate = jnp.sum(out_rate * pi_lane[0:1], axis=1, keepdims=True)
    gen = (off - jnp.where(sub == lane, out_rate, 0.0)) / mean_rate

    def times(left, right):
        acc = left[:, 0:1] * right[0:1, :]
        for mid in range(1, STATES):
            acc = acc + left[:, mid : mid + 1] * right[mid : mid + 1, :]
        return acc

    second = times(gen, gen) * 0.5
    third = times(second, gen) * (1.0 / 3.0)
    fourth = times(second, second) * (4.0 / 24.0)
    powers = [gen, second, third, fourth]
    for order, part in ((5, gen), (6, second), (7, third), (8, fourth)):
        ratio = {5: 24.0 / 120.0, 6: 48.0 / 720.0, 7: 144.0 / 5040.0, 8: 576.0 / 40320.0}[order]
        powers.append(times(fourth, part) * ratio)
    return powers, pi_sub


def taylor(powers, rates_ref, branch_ref, mat_ref):
    shape = (1, LANES)
    lane = iota(shape, 1)
    category = lane // SPLIT
    rate = jnp.zeros(shape, F32)
    mean = jnp.zeros(shape, F32)
    for k in range(RATES):
        rate = jnp.where(category == k, rates_ref[k], rate)
        mean = mean + rates_ref[k]
    rate = rate / (mean / RATES)
    taus = []
    for half in range(2):
        length = jnp.zeros(shape, F32)
        for at in range(min(SPLIT, NODES - half * SPLIT)):
            length = jnp.where(lane % SPLIT == at, branch_ref[half * SPLIT + at], length)
        taus.append(length * rate / 256.0)
    sub = iota((PAD, LANES), 0)
    for i in range(STATES):
        columns = [jnp.broadcast_to(p[:, i : i + 1], (PAD, LANES)) for p in powers]
        eye = jnp.where(sub == i, 1.0, 0.0)
        for half in range(2):
            acc = columns[7]
            for order in range(6, -1, -1):
                acc = columns[order] + acc * taus[half]
            mat_ref[0, half, i * PAD : (i + 1) * PAD, :] = eye + acc * taus[half]


def square(step, half, mat_ref, beside=None):
    src = lax.rem(step, 2)
    dst = 1 - src
    for first in range(0, STATES, 4):
        if beside is not None:
            beside(first // 4)
        accs = [None] * 4
        for mid in range(STATES):
            row = mat_ref[src, half, mid * PAD : (mid + 1) * PAD, :]
            for at in range(4):
                where = (first + at) * PAD + mid
                factor = mat_ref[src, half, where : where + 1, :]
                term = factor * row
                accs[at] = term if accs[at] is None else accs[at] + term
        for at in range(4):
            start = (first + at) * PAD
            mat_ref[dst, half, start : start + PAD, :] = accs[at]


def tree_order(children_ref, order_ref):
    place = NODES
    parents = [NODES]
    for count in (2, 4, 8, 16, 32):
        place = place - count
        ids = []
        for at, parent in enumerate(parents):
            row = jnp.clip(parent - LEAVES, 0, NODES - LEAVES)
            for side in range(2):
                child = children_ref[side, row]
                order_ref[place + 2 * at + side] = child
                ids.append(child)
        parents = ids


def spread(half, mat_ref, spread_ref):
    for group in range(4):
        block = mat_ref[0, half, group * 120 : group * 120 + LANES, :].T
        for at in range(5):
            i = group * 5 + at
            moved = block if at == 0 else pltpu.roll(block, LANES - PAD * at, 1)
            for k in range(RATES):
                rows = pl.ds(i * RATES + k, SPLIT, stride=SPREAD)
                spread_ref[half, rows, :] = moved[k * SPLIT : (k + 1) * SPLIT]


def parts(half, at, spread_ref):
    value = spread_ref[half, pl.ds(at * SPREAD, ROWS), :]
    value = jnp.where(iota((ROWS, LANES), 1) < STATES, value, 0.0)
    high = value.astype(BF16).astype(F32)
    return high, value - high


def leaf_operands(order_ref, spread_ref, leaf_ref):
    for node in range(LEAVES // 2):
        high, low = parts(0, jnp.clip(order_ref[2 * node], 0, LEAVES - 1), spread_ref)
        leaf_ref[node, 0:ROWS, :] = (high + pltpu.roll(low, 32, 1)).astype(BF16)
        high, low = parts(0, jnp.clip(order_ref[2 * node + 1], 0, LEAVES - 1), spread_ref)
        leaf_ref[node, ROWS : 2 * ROWS, :] = (
            pltpu.roll(high, 64, 1) + pltpu.roll(low, 96, 1)
        ).astype(BF16)


def inner_operands(order_ref, spread_ref, inner_ref):
    row, col = iota((LANES, 256), 0), iota((LANES, 256), 1)
    state = lax.rem(col, ROWS) // RATES
    low_part = (col >= 2 * ROWS).astype(jnp.int32) * 32
    place = jnp.where((row == state + low_part) & (col < 3 * ROWS), 1.0, 0.0).astype(BF16)
    row, col = iota((ROWS, 256), 0), iota((ROWS, 256), 1)
    same = lax.rem(row, RATES) == lax.rem(col, RATES)
    for at in range(INNER):
        child = jnp.clip(order_ref[LEAVES + at] - LEAVES, 0, INNER - 1)
        high, low = parts(1, child, spread_ref)
        both = (high + pltpu.roll(low, 32, 1)).astype(BF16)
        wide = jnp.dot(both, place, preferred_element_type=F32)
        inner_ref[at] = jnp.where(same, wide, 0.0).astype(BF16)


def gather_leaves(chunk, tips_ref, order_ref, flat_ref, leaves_ref):
    tiles = CHUNK // LANES
    for tile in range(tiles):
        lanes = pl.ds(pl.multiple_of(chunk * CHUNK, CHUNK) + tile * LANES, LANES)
        for state in range(STATES):
            rows = pl.ds(state, LEAVES, stride=FLAT)
            flat_ref[tile, rows, :] = tips_ref[state, :, lanes].astype(F32)
    filler = jnp.zeros((SPLIT - PAD, CHUNK), F32)
    for at in range(LEAVES):
        rows = pl.ds(jnp.clip(order_ref[at], 0, LEAVES - 1) * FLAT, PAD)
        value = jnp.concatenate([flat_ref[tile, rows, :] for tile in range(tiles)], axis=1)
        value = jnp.concatenate([value, filler], axis=0).astype(BF16)
        leaves_ref[chunk, at * SPLIT : (at + 1) * SPLIT, :] = value


def keep(ref, chunk, at, value):
    high = value.astype(BF16)
    ref[chunk, at, 0:ROWS, :] = high
    ref[chunk, at, ROWS : 2 * ROWS, :] = (value - high.astype(F32)).astype(BF16)


def prune_leaves(nodes, chunk, leaves_ref, leaf_ref, level_ref):
    for node in nodes:
        left = leaves_ref[chunk, 2 * node * SPLIT : (2 * node + 1) * SPLIT, :]
        right = leaves_ref[chunk, (2 * node + 1) * SPLIT : (2 * node + 2) * SPLIT, :]
        stacked = jnp.concatenate([left, left, right, right], axis=0)
        both = jnp.dot(leaf_ref[node], stacked, preferred_element_type=F32)
        keep(level_ref, chunk, node, both[0:ROWS] * both[ROWS:])


def prune_inner(chunks, inner_ref, level_refs, weight):
    def moved(at, ref, chunk, child):
        high = ref[chunk, child, 0:ROWS, :]
        low = ref[chunk, child, ROWS : 2 * ROWS, :]
        stacked = jnp.concatenate([high, low, high], axis=0)
        return jnp.dot(inner_ref[at, :, 0 : 3 * ROWS], stacked, preferred_element_type=F32)

    scales = [jnp.zeros((1, CHUNK), F32) for _ in range(chunks)]
    results = []
    base = 0
    for level, count in enumerate(LEVEL_NODES):
        ref = level_refs[level]
        parents = count // 2
        for chunk in range(chunks):
            for place in range(parents):
                at = base + 2 * place
                value = moved(at, ref, chunk, 2 * place) * moved(at + 1, ref, chunk, 2 * place + 1)
                if parents == 4:
                    top = jnp.max(value, axis=0, keepdims=True)
                    value = value * (1.0 / top)
                    scales[chunk] = scales[chunk] + jnp.log(top)
                if parents > 1:
                    keep(level_refs[level + 1], chunk, place, value)
                else:
                    lik = jnp.sum(value * weight, axis=0, keepdims=True)
                    results.append(jnp.log(lik) + scales[chunk])
        base = base + count
    return results


def peers(genes, sites):
    return [(g, m) for g in range(genes) for m in range(sites) if g or m]


def kernel(
    mesh_shape,
    scale,
    children_ref,
    gene_ref,
    count_ref,
    freqs_ref,
    rates_ref,
    branch_ref,
    exchange_ref,
    tips_hbm,
    site_ref,
    mean_ref,
    total_ref,
    tips_ref,
    order_ref,
    leaves_ref,
    pad_ref,
    mat_ref,
    spread_ref,
    leaf_ref,
    inner_ref,
    flat_ref,
    level_refs,
    weight_ref,
    part_ref,
    rows_ref,
    fetch_sems,
    sems,
):
    genes, sites = mesh_shape
    barrier = pltpu.get_barrier_semaphore()
    group, member = lax.axis_index("gene"), lax.axis_index("site")

    def device(gene, site):
        return (lax.rem(group + gene, genes), lax.rem(member + site, sites))

    for gene, site in peers(genes, sites):
        pl.semaphore_signal(barrier, inc=1, device_id=device(gene, site))
    chunks = site_ref.shape[1] // CHUNK

    def fetch(chunk):
        lanes = pl.ds(pl.multiple_of(chunk * CHUNK, CHUNK), CHUNK)
        return pltpu.make_async_copy(
            tips_hbm.at[0, :, :, lanes], tips_ref.at[:, :, lanes], fetch_sems.at[chunk]
        )

    for chunk in range(chunks):
        fetch(chunk).start()
    tree_order(children_ref, order_ref)
    for tile in range(CHUNK // LANES):
        flat_ref[tile] = jnp.zeros((LEAVES * FLAT, LANES), F32)
    powers, pi_sub = rate_powers(exchange_ref, freqs_ref, pad_ref)
    for i in range(STATES):
        row = jnp.broadcast_to(pi_sub[i : i + 1, 0:1] / RATES, (RATES, LANES))
        weight_ref[i * RATES : (i + 1) * RATES, :] = row

    taylor(powers, rates_ref, branch_ref, mat_ref)
    per_step = chunks // SQUARINGS

    def leaf_branches(step, carry):
        for at in range(per_step):
            chunk = step * per_step + at
            fetch(chunk).wait()
            gather_leaves(chunk, tips_ref, order_ref, flat_ref, leaves_ref)
        square(step, 0, mat_ref)
        return carry

    lax.fori_loop(0, SQUARINGS, leaf_branches, 0)
    spread(0, mat_ref, spread_ref)
    leaf_operands(order_ref, spread_ref, leaf_ref)

    def inner_branches(step, carry):
        def beside(number):
            for at in range(per_step):
                nodes = range(LEAVES // 2 * number // 5, LEAVES // 2 * (number + 1) // 5)
                prune_leaves(nodes, step * per_step + at, leaves_ref, leaf_ref, level_refs[0])

        square(step, 1, mat_ref, beside)
        return carry

    lax.fori_loop(0, SQUARINGS, inner_branches, 0)
    spread(1, mat_ref, spread_ref)
    inner_operands(order_ref, spread_ref, inner_ref)
    results = prune_inner(chunks, inner_ref, level_refs, weight_ref[:, 0:1])
    lane = iota((1, LANES), 1)
    gathered = jnp.zeros((1, LANES), F32)
    for slot in range(chunks * CHUNK // LANES):
        live = count_ref[0, slot]
        gene = gene_ref[0, slot]
        at = slot * LANES % CHUNK
        part = results[slot * LANES // CHUNK][:, at : at + LANES]
        part = jnp.where(lane < live, part, 0.0)
        site_ref[:, slot * LANES : (slot + 1) * LANES] = part
        summed = jnp.sum(part, axis=1, keepdims=True)
        gathered = gathered + jnp.where(lane == gene, summed, 0.0)
        gathered = gathered + jnp.where(lane == gene + GENES, live.astype(F32), 0.0)
    part_ref[...] = gathered
    pl.semaphore_wait(barrier, genes * sites - 1)
    copies = []
    for gene, site in peers(genes, sites):
        at = gene * sites + site
        copies.append(
            pltpu.make_async_remote_copy(
                src_ref=part_ref,
                dst_ref=rows_ref.at[group, member],
                send_sem=sems.at[0, at],
                recv_sem=sems.at[1, at],
                device_id=device(gene, site),
            )
        )
    for copy in copies:
        copy.start()
    rows_ref[group, member] = gathered
    for copy in copies:
        copy.wait()
    summed = rows_ref[group, 0]
    for at in range(1, sites):
        summed = summed + rows_ref[group, at]
    mean_ref[...] = (summed / pltpu.roll(summed, GENES, 1))[:, 0:GENES]
    total = jnp.zeros((1, LANES), F32)
    for gene in range(genes):
        for site in range(sites):
            total = total + rows_ref[gene, site]
    total = jnp.sum(jnp.where(lane < GENES, total, 0.0), axis=1, keepdims=True)
    total_ref[...] = total * (1.0 / scale)


def likelihoods(genes, width, tips, exchange_, freqs, rates, branch, children, slot_gene, site_count):
    sites = tips.shape[3]
    chunks = sites // CHUNK
    smem = pl.BlockSpec(memory_space=pltpu.SMEM)
    vmem = pl.BlockSpec(memory_space=pltpu.VMEM)
    return pl.pallas_call(
        functools.partial(kernel, (genes, width), sites * width),
        name="likelihoods",
        out_shape=(
            jax.ShapeDtypeStruct((1, sites), F32),
            jax.ShapeDtypeStruct((1, GENES), F32),
            jax.ShapeDtypeStruct((1, 1), F32),
        ),
        in_specs=[smem] * 6 + [vmem, pl.BlockSpec(memory_space=pl.ANY)],
        out_specs=(vmem, vmem, vmem),
        scratch_shapes=[
            pltpu.VMEM((STATES, LEAVES, sites), BF16),
            pltpu.SMEM((NODES,), jnp.int32),
            pltpu.VMEM((chunks, LEAVES * SPLIT, CHUNK), BF16),
            pltpu.VMEM((LANES, LANES), F32),
            pltpu.VMEM((2, 2, 512, LANES), F32),
            pltpu.VMEM((2, SPLIT * SPREAD, LANES), F32),
            pltpu.VMEM((LEAVES // 2, 2 * ROWS, LANES), BF16),
            pltpu.VMEM((INNER, ROWS, 256), BF16),
            pltpu.VMEM((CHUNK // LANES, FLAT * LEAVES, LANES), F32),
            [pltpu.VMEM((chunks, count, 2 * ROWS, CHUNK), BF16) for count in LEVEL_NODES],
            pltpu.VMEM((ROWS, LANES), F32),
            pltpu.VMEM((1, LANES), F32),
            pltpu.VMEM((genes, width, 1, LANES), F32),
            pltpu.SemaphoreType.DMA((chunks,)),
            pltpu.SemaphoreType.DMA((2, genes * width)),
        ],
        compiler_params=pltpu.CompilerParams(
            vmem_limit_bytes=60 * 1024 * 1024, collective_id=0, has_side_effects=True
        ),
    )(
        children.T,
        slot_gene,
        site_count,
        freqs,
        rates,
        branch,
        exchange_,
        tips.transpose(0, 2, 1, 3),
    )


def solution(mesh):
    genes, sites = mesh.shape["gene"], mesh.shape["site"]

    def on_device(*args):
        values, gene_loglik, total = likelihoods(genes, sites, *args)
        return values, gene_loglik, total.reshape(())

    pair = P("gene", "site")
    return jax.shard_map(
        on_device,
        mesh=mesh,
        in_specs=(P("gene", None, None, "site"), P(), P(), P(), P(), P(), pair, pair),
        out_specs=(pair, P("gene", None), P()),
        check_vma=False,
    )
```

```python
import functools

import jax
import jax.numpy as jnp
from jax import lax
from jax.experimental import pallas as pl
from jax.experimental.pallas import tpu as pltpu
from jax.sharding import PartitionSpec as P

STATES = 20
RATES = 4
ROWS = STATES * RATES
LEAVES = 32
INNER = 30
NODES = 62
GENES = 64
PAD = 24
LANES = 128
SPLIT = 32
CHUNK = 256
LEVEL_NODES = (16, 8, 4, 2)
SQUARINGS = 8
SPREAD = ROWS + 1
FLAT = PAD + 1
F32 = jnp.float32
BF16 = jnp.bfloat16


def iota(shape, axis):
    return lax.broadcasted_iota(jnp.int32, shape, axis)


def rate_powers(exchange_ref, freqs_ref, pad_ref):
    pad_ref[...] = jnp.zeros((LANES, LANES), F32)
    pad_ref[0:STATES, 0:STATES] = exchange_ref[...]
    full = pad_ref[...]
    both = (full + full.T)[0:PAD, :]
    shape = (PAD, LANES)
    sub, lane = iota(shape, 0), iota(shape, 1)
    pi_sub = jnp.zeros(shape, F32)
    pi_lane = jnp.zeros(shape, F32)
    for state in range(STATES):
        value = freqs_ref[state]
        pi_sub = jnp.where(sub == state, value, pi_sub)
        pi_lane = jnp.where(lane == state, value, pi_lane)
    total = jnp.sum(pi_sub, axis=0, keepdims=True)
    pi_sub = pi_sub / total
    pi_lane = pi_lane / total
    off = jnp.where(sub == lane, 0.0, both * 0.5 * pi_sub)
    out_rate = jnp.sum(off, axis=0, keepdims=True)
    mean_rate = jnp.sum(out_rate * pi_lane[0:1], axis=1, keepdims=True)
    gen = (off - jnp.where(sub == lane, out_rate, 0.0)) / mean_rate

    def times(left, right):
        acc = left[:, 0:1] * right[0:1, :]
        for mid in range(1, STATES):
            acc = acc + left[:, mid : mid + 1] * right[mid : mid + 1, :]
        return acc

    second = times(gen, gen) * 0.5
    third = times(second, gen) * (1.0 / 3.0)
    fourth = times(second, second) * (4.0 / 24.0)
    powers = [gen, second, third, fourth]
    for order, part in ((5, gen), (6, second), (7, third), (8, fourth)):
        ratio = {5: 24.0 / 120.0, 6: 48.0 / 720.0, 7: 144.0 / 5040.0, 8: 576.0 / 40320.0}[order]
        powers.append(times(fourth, part) * ratio)
    return powers, pi_sub


def taylor(powers, rates_ref, branch_ref, mat_ref):
    shape = (1, LANES)
    lane = iota(shape, 1)
    category = lane // SPLIT
    rate = jnp.zeros(shape, F32)
    mean = jnp.zeros(shape, F32)
    for k in range(RATES):
        rate = jnp.where(category == k, rates_ref[k], rate)
        mean = mean + rates_ref[k]
    rate = rate / (mean / RATES)
    taus = []
    for half in range(2):
        length = jnp.zeros(shape, F32)
        for at in range(min(SPLIT, NODES - half * SPLIT)):
            length = jnp.where(lane % SPLIT == at, branch_ref[half * SPLIT + at], length)
        taus.append(length * rate / 256.0)
    sub = iota((PAD, LANES), 0)
    for i in range(STATES):
        columns = [jnp.broadcast_to(p[:, i : i + 1], (PAD, LANES)) for p in powers]
        eye = jnp.where(sub == i, 1.0, 0.0)
        for half in range(2):
            acc = columns[7]
            for order in range(6, -1, -1):
                acc = columns[order] + acc * taus[half]
            mat_ref[0, half, i * PAD : (i + 1) * PAD, :] = eye + acc * taus[half]


def square(step, half, mat_ref, beside=None):
    src = lax.rem(step, 2)
    dst = 1 - src
    for first in range(0, STATES, 4):
        if beside is not None:
            beside(first // 4)
        accs = [None] * 4
        for mid in range(STATES):
            row = mat_ref[src, half, mid * PAD : (mid + 1) * PAD, :]
            for at in range(4):
                where = (first + at) * PAD + mid
                factor = mat_ref[src, half, where : where + 1, :]
                term = factor * row
                accs[at] = term if accs[at] is None else accs[at] + term
        for at in range(4):
            start = (first + at) * PAD
            mat_ref[dst, half, start : start + PAD, :] = accs[at]


def tree_order(children_ref, order_ref):
    place = NODES
    parents = [NODES]
    for count in (2, 4, 8, 16, 32):
        place = place - count
        ids = []
        for at, parent in enumerate(parents):
            row = jnp.clip(parent - LEAVES, 0, NODES - LEAVES)
            for side in range(2):
                child = children_ref[side, row]
                order_ref[place + 2 * at + side] = child
                ids.append(child)
        parents = ids


def spread(half, mat_ref, spread_ref):
    for group in range(4):
        block = mat_ref[0, half, group * 120 : group * 120 + LANES, :].T
        for at in range(5):
            i = group * 5 + at
            moved = block if at == 0 else pltpu.roll(block, LANES - PAD * at, 1)
            for k in range(RATES):
                rows = pl.ds(i * RATES + k, SPLIT, stride=SPREAD)
                spread_ref[half, rows, :] = moved[k * SPLIT : (k + 1) * SPLIT]


def parts(half, at, spread_ref):
    value = spread_ref[half, pl.ds(at * SPREAD, ROWS), :]
    value = jnp.where(iota((ROWS, LANES), 1) < STATES, value, 0.0)
    high = value.astype(BF16).astype(F32)
    return high, value - high


def leaf_operands(order_ref, spread_ref, leaf_ref):
    for node in range(LEAVES // 2):
        high, low = parts(0, jnp.clip(order_ref[2 * node], 0, LEAVES - 1), spread_ref)
        leaf_ref[node, 0:ROWS, :] = (high + pltpu.roll(low, 32, 1)).astype(BF16)
        high, low = parts(0, jnp.clip(order_ref[2 * node + 1], 0, LEAVES - 1), spread_ref)
        leaf_ref[node, ROWS : 2 * ROWS, :] = (
            pltpu.roll(high, 64, 1) + pltpu.roll(low, 96, 1)
        ).astype(BF16)


def inner_operands(order_ref, spread_ref, inner_ref):
    row, col = iota((LANES, 256), 0), iota((LANES, 256), 1)
    state = lax.rem(col, ROWS) // RATES
    low_part = (col >= 2 * ROWS).astype(jnp.int32) * 32
    place = jnp.where((row == state + low_part) & (col < 3 * ROWS), 1.0, 0.0).astype(BF16)
    row, col = iota((ROWS, 256), 0), iota((ROWS, 256), 1)
    same = lax.rem(row, RATES) == lax.rem(col, RATES)
    for at in range(INNER):
        child = jnp.clip(order_ref[LEAVES + at] - LEAVES, 0, INNER - 1)
        high, low = parts(1, child, spread_ref)
        both = (high + pltpu.roll(low, 32, 1)).astype(BF16)
        wide = jnp.dot(both, place, preferred_element_type=F32)
        inner_ref[at] = jnp.where(same, wide, 0.0).astype(BF16)


def gather_leaves(chunk, tips_ref, order_ref, flat_ref, leaves_ref):
    tiles = CHUNK // LANES
    for tile in range(tiles):
        lanes = pl.ds(pl.multiple_of(chunk * CHUNK, CHUNK) + tile * LANES, LANES)
        for state in range(STATES):
            rows = pl.ds(state, LEAVES, stride=FLAT)
            flat_ref[tile, rows, :] = tips_ref[state, :, lanes].astype(F32)
    filler = jnp.zeros((SPLIT - PAD, CHUNK), F32)
    for at in range(LEAVES):
        rows = pl.ds(jnp.clip(order_ref[at], 0, LEAVES - 1) * FLAT, PAD)
        value = jnp.concatenate([flat_ref[tile, rows, :] for tile in range(tiles)], axis=1)
        value = jnp.concatenate([value, filler], axis=0).astype(BF16)
        leaves_ref[chunk, at * SPLIT : (at + 1) * SPLIT, :] = value


def keep(ref, chunk, at, value):
    high = value.astype(BF16)
    ref[chunk, at, 0:ROWS, :] = high
    ref[chunk, at, ROWS : 2 * ROWS, :] = (value - high.astype(F32)).astype(BF16)


def prune_leaves(nodes, chunk, leaves_ref, leaf_ref, level_ref):
    for node in nodes:
        left = leaves_ref[chunk, 2 * node * SPLIT : (2 * node + 1) * SPLIT, :]
        right = leaves_ref[chunk, (2 * node + 1) * SPLIT : (2 * node + 2) * SPLIT, :]
        stacked = jnp.concatenate([left, left, right, right], axis=0)
        both = jnp.dot(leaf_ref[node], stacked, preferred_element_type=F32)
        keep(level_ref, chunk, node, both[0:ROWS] * both[ROWS:])


def prune_inner(chunks, inner_ref, level_refs, weight):
    def moved(at, ref, chunk, child):
        high = ref[chunk, child, 0:ROWS, :]
        low = ref[chunk, child, ROWS : 2 * ROWS, :]
        stacked = jnp.concatenate([high, low, high], axis=0)
        return jnp.dot(inner_ref[at, :, 0 : 3 * ROWS], stacked, preferred_element_type=F32)

    scales = [jnp.zeros((1, CHUNK), F32) for _ in range(chunks)]
    results = []
    base = 0
    for level, count in enumerate(LEVEL_NODES):
        ref = level_refs[level]
        parents = count // 2
        for chunk in range(chunks):
            for place in range(parents):
                at = base + 2 * place
                value = moved(at, ref, chunk, 2 * place) * moved(at + 1, ref, chunk, 2 * place + 1)
                if parents == 4:
                    top = jnp.max(value, axis=0, keepdims=True)
                    value = value * (1.0 / top)
                    scales[chunk] = scales[chunk] + jnp.log(top)
                if parents > 1:
                    keep(level_refs[level + 1], chunk, place, value)
                else:
                    lik = jnp.sum(value * weight, axis=0, keepdims=True)
                    results.append(jnp.log(lik) + scales[chunk])
        base = base + count
    return results


def exchange(axis, size, own_ref, buf, send, recv):
    me = lax.axis_index(axis)
    copies = []
    for off in range(1, size):
        copies.append(
            pltpu.make_async_remote_copy(
                src_ref=own_ref,
                dst_ref=buf.at[me],
                send_sem=send.at[off],
                recv_sem=recv.at[off],
                device_id={axis: lax.rem(me + off, size)},
            )
        )
    for copy in copies:
        copy.start()
    buf[me] = own_ref[...]
    return copies


def total_of(copies, buf, size):
    for copy in copies:
        copy.wait()
    summed = buf[0]
    for at in range(1, size):
        summed = summed + buf[at]
    return summed


def kernel(
    mesh_shape,
    children_ref,
    gene_ref,
    count_ref,
    freqs_ref,
    rates_ref,
    branch_ref,
    exchange_ref,
    tips_hbm,
    site_ref,
    sums_ref,
    total_ref,
    tips_ref,
    order_ref,
    leaves_ref,
    pad_ref,
    mat_ref,
    spread_ref,
    leaf_ref,
    inner_ref,
    flat_ref,
    level_refs,
    weight_ref,
    part_ref,
    own_ref,
    site_buf,
    gene_buf,
    fetch_sems,
    site_sems,
    gene_sems,
):
    genes, sites = mesh_shape
    barrier = pltpu.get_barrier_semaphore()
    for axis, size in (("site", sites), ("gene", genes)):
        for off in range(1, size):
            peer = lax.rem(lax.axis_index(axis) + off, size)
            pl.semaphore_signal(barrier, inc=1, device_id={axis: peer})
    chunks = site_ref.shape[1] // CHUNK

    def fetch(chunk):
        lanes = pl.ds(pl.multiple_of(chunk * CHUNK, CHUNK), CHUNK)
        return pltpu.make_async_copy(
            tips_hbm.at[0, :, :, lanes], tips_ref.at[:, :, lanes], fetch_sems.at[chunk]
        )

    for chunk in range(chunks):
        fetch(chunk).start()
    tree_order(children_ref, order_ref)
    for tile in range(CHUNK // LANES):
        flat_ref[tile] = jnp.zeros((LEAVES * FLAT, LANES), F32)
    powers, pi_sub = rate_powers(exchange_ref, freqs_ref, pad_ref)
    for i in range(STATES):
        row = jnp.broadcast_to(pi_sub[i : i + 1, 0:1] / RATES, (RATES, LANES))
        weight_ref[i * RATES : (i + 1) * RATES, :] = row

    taylor(powers, rates_ref, branch_ref, mat_ref)
    per_step = chunks // SQUARINGS

    def leaf_branches(step, carry):
        for at in range(per_step):
            chunk = step * per_step + at
            fetch(chunk).wait()
            gather_leaves(chunk, tips_ref, order_ref, flat_ref, leaves_ref)
        square(step, 0, mat_ref)
        return carry

    lax.fori_loop(0, SQUARINGS, leaf_branches, 0)
    spread(0, mat_ref, spread_ref)
    leaf_operands(order_ref, spread_ref, leaf_ref)

    def inner_branches(step, carry):
        def beside(number):
            for at in range(per_step):
                nodes = range(LEAVES // 2 * number // 5, LEAVES // 2 * (number + 1) // 5)
                prune_leaves(nodes, step * per_step + at, leaves_ref, leaf_ref, level_refs[0])

        square(step, 1, mat_ref, beside)
        return carry

    lax.fori_loop(0, SQUARINGS, inner_branches, 0)
    spread(1, mat_ref, spread_ref)
    inner_operands(order_ref, spread_ref, inner_ref)
    results = prune_inner(chunks, inner_ref, level_refs, weight_ref[:, 0:1])
    lane = iota((1, LANES), 1)
    gathered = jnp.zeros((1, LANES), F32)
    for slot in range(chunks * CHUNK // LANES):
        live = count_ref[0, slot]
        gene = gene_ref[0, slot]
        at = slot * LANES % CHUNK
        part = results[slot * LANES // CHUNK][:, at : at + LANES]
        part = jnp.where(lane < live, part, 0.0)
        site_ref[:, slot * LANES : (slot + 1) * LANES] = part
        summed = jnp.sum(part, axis=1, keepdims=True)
        gathered = gathered + jnp.where(lane == gene, summed, 0.0)
        gathered = gathered + jnp.where(lane == gene + GENES, live.astype(F32), 0.0)
    part_ref[...] = gathered
    pl.semaphore_wait(barrier, sites + genes - 2)
    copies = exchange("site", sites, part_ref, site_buf, site_sems.at[0], site_sems.at[1])
    summed = total_of(copies, site_buf, sites)
    own = jnp.sum(jnp.where(lane < GENES, summed, 0.0), axis=1, keepdims=True)
    own_ref[...] = jnp.broadcast_to(own, (1, LANES))
    copies = exchange("gene", genes, own_ref, gene_buf, gene_sems.at[0], gene_sems.at[1])
    sums_ref[...] = summed
    total_ref[...] = total_of(copies, gene_buf, genes)


def likelihoods(genes, width, tips, exchange_, freqs, rates, branch, children, slot_gene, site_count):
    sites = tips.shape[3]
    chunks = sites // CHUNK
    smem = pl.BlockSpec(memory_space=pltpu.SMEM)
    vmem = pl.BlockSpec(memory_space=pltpu.VMEM)
    return pl.pallas_call(
        functools.partial(kernel, (genes, width)),
        name="likelihoods",
        out_shape=(
            jax.ShapeDtypeStruct((1, sites), F32),
            jax.ShapeDtypeStruct((1, LANES), F32),
            jax.ShapeDtypeStruct((1, LANES), F32),
        ),
        in_specs=[smem] * 6 + [vmem, pl.BlockSpec(memory_space=pl.ANY)],
        out_specs=(vmem, vmem, vmem),
        scratch_shapes=[
            pltpu.VMEM((STATES, LEAVES, sites), BF16),
            pltpu.SMEM((NODES,), jnp.int32),
            pltpu.VMEM((chunks, LEAVES * SPLIT, CHUNK), BF16),
            pltpu.VMEM((LANES, LANES), F32),
            pltpu.VMEM((2, 2, 512, LANES), F32),
            pltpu.VMEM((2, SPLIT * SPREAD, LANES), F32),
            pltpu.VMEM((LEAVES // 2, 2 * ROWS, LANES), BF16),
            pltpu.VMEM((INNER, ROWS, 256), BF16),
            pltpu.VMEM((CHUNK // LANES, FLAT * LEAVES, LANES), F32),
            [pltpu.VMEM((chunks, count, 2 * ROWS, CHUNK), BF16) for count in LEVEL_NODES],
            pltpu.VMEM((ROWS, LANES), F32),
            pltpu.VMEM((1, LANES), F32),
            pltpu.VMEM((1, LANES), F32),
            pltpu.VMEM((width, 1, LANES), F32),
            pltpu.VMEM((genes, 1, LANES), F32),
            pltpu.SemaphoreType.DMA((chunks,)),
            pltpu.SemaphoreType.DMA((2, width)),
            pltpu.SemaphoreType.DMA((2, genes)),
        ],
        compiler_params=pltpu.CompilerParams(
            vmem_limit_bytes=60 * 1024 * 1024, collective_id=0, has_side_effects=True
        ),
    )(
        children.T,
        slot_gene,
        site_count,
        freqs,
        rates,
        branch,
        exchange_,
        tips.transpose(0, 2, 1, 3),
    )


def finish_kernel(scale, values_ref, sums_ref, total_ref, site_out, mean_out, total_out):
    site_out[...] = values_ref[...]
    sums = sums_ref[...]
    mean_out[...] = (sums / pltpu.roll(sums, GENES, 1))[:, 0:GENES]
    total_out[...] = total_ref[:, 0:1] * (1.0 / scale)


def finish(values, sums, total, scale):
    vmem = pl.BlockSpec(memory_space=pltpu.VMEM)
    return pl.pallas_call(
        functools.partial(finish_kernel, scale),
        name="finish",
        out_shape=(
            jax.ShapeDtypeStruct(values.shape, F32),
            jax.ShapeDtypeStruct((1, GENES), F32),
            jax.ShapeDtypeStruct((1, 1), F32),
        ),
        in_specs=[vmem] * 3,
        out_specs=(vmem, vmem, vmem),
    )(values, sums, total)


def solution(mesh):
    genes, sites = mesh.shape["gene"], mesh.shape["site"]

    def on_device(*args):
        values, sums, total = likelihoods(genes, sites, *args)
        scale = values.shape[1] * sites
        values, gene_loglik, total = finish(values, sums, total, scale)
        return values, gene_loglik, total.reshape(())

    pair = P("gene", "site")
    return jax.shard_map(
        on_device,
        mesh=mesh,
        in_specs=(P("gene", None, None, "site"), P(), P(), P(), P(), P(), pair, pair),
        out_specs=(pair, P("gene", None), P()),
        check_vma=False,
    )
```

```python
import functools

import jax
import jax.numpy as jnp
from jax import lax
from jax.experimental import pallas as pl
from jax.experimental.pallas import tpu as pltpu
from jax.sharding import PartitionSpec as P

STATES = 20
RATES = 4
ROWS = STATES * RATES
LEAVES = 32
INNER = 30
NODES = 62
GENES = 64
PAD = 24
LANES = 128
SPLIT = 32
CHUNK = 256
LEVEL_NODES = (16, 8, 4, 2)
SQUARINGS = 8
SPREAD = ROWS + 1
FLAT = PAD + 1
F32 = jnp.float32
BF16 = jnp.bfloat16


def iota(shape, axis):
    return lax.broadcasted_iota(jnp.int32, shape, axis)


def rate_powers(exchange_ref, freqs_ref, pad_ref):
    pad_ref[...] = jnp.zeros((LANES, LANES), F32)
    pad_ref[0:STATES, 0:STATES] = exchange_ref[...]
    full = pad_ref[...]
    both = (full + full.T)[0:PAD, :]
    shape = (PAD, LANES)
    sub, lane = iota(shape, 0), iota(shape, 1)
    pi_sub = jnp.zeros(shape, F32)
    pi_lane = jnp.zeros(shape, F32)
    for state in range(STATES):
        value = freqs_ref[state]
        pi_sub = jnp.where(sub == state, value, pi_sub)
        pi_lane = jnp.where(lane == state, value, pi_lane)
    total = jnp.sum(pi_sub, axis=0, keepdims=True)
    pi_sub = pi_sub / total
    pi_lane = pi_lane / total
    sym = jnp.where(sub == lane, 0.0, both * 0.5)
    out_rate = jnp.sum(sym * pi_sub, axis=0, keepdims=True)
    mean_rate = jnp.sum(out_rate * pi_lane[0:1], axis=1, keepdims=True)
    root_sub, root_lane = jnp.sqrt(pi_sub), jnp.sqrt(pi_lane)
    gen = (sym * root_sub * root_lane - jnp.where(sub == lane, out_rate, 0.0)) / mean_rate

    def times(left, right):
        acc = left[:, 0:1] * right[0:1, :]
        for mid in range(1, STATES):
            acc = acc + left[:, mid : mid + 1] * right[mid : mid + 1, :]
        return acc

    second = times(gen, gen) * 0.5
    third = times(second, gen) * (1.0 / 3.0)
    fourth = times(second, second) * (4.0 / 24.0)
    powers = [gen, second, third, fourth]
    for order, part in ((5, gen), (6, second), (7, third), (8, fourth)):
        ratio = {5: 24.0 / 120.0, 6: 48.0 / 720.0, 7: 144.0 / 5040.0, 8: 576.0 / 40320.0}[order]
        powers.append(times(fourth, part) * ratio)
    return powers, pi_sub


def taylor(powers, rates_ref, branch_ref, mat_ref):
    shape = (1, LANES)
    lane = iota(shape, 1)
    category = lane // SPLIT
    rate = jnp.zeros(shape, F32)
    mean = jnp.zeros(shape, F32)
    for k in range(RATES):
        rate = jnp.where(category == k, rates_ref[k], rate)
        mean = mean + rates_ref[k]
    rate = rate / (mean / RATES)
    taus = []
    for half in range(2):
        length = jnp.zeros(shape, F32)
        for at in range(min(SPLIT, NODES - half * SPLIT)):
            length = jnp.where(lane % SPLIT == at, branch_ref[half * SPLIT + at], length)
        taus.append(length * rate / 256.0)
    sub = iota((PAD, LANES), 0)
    for i in range(STATES):
        columns = [jnp.broadcast_to(p[:, i : i + 1], (PAD, LANES)) for p in powers]
        eye = jnp.where(sub == i, 1.0, 0.0)
        for half in range(2):
            acc = columns[7]
            for order in range(6, -1, -1):
                acc = columns[order] + acc * taus[half]
            mat_ref[0, half, i * FLAT : i * FLAT + PAD, :] = eye + acc * taus[half]


def rows_of(src, half, mid, group, mat_ref):
    if group >= mid // 8:
        return mat_ref[src, half, pl.ds(mid * FLAT + 8 * group, 8), :]
    return mat_ref[src, half, pl.ds(8 * group * FLAT + mid, 8, stride=FLAT), :]


def square(step, half, mat_ref, whole, beside=None):
    src = lax.rem(step, 2)
    dst = 1 - src
    for first in range(0, STATES, 4):
        if beside is not None:
            beside(first // 4)
        groups = range(0 if whole is not None else first // 8, PAD // 8)
        accs = {}
        for mid in range(STATES):
            rows = {group: rows_of(src, half, mid, group, mat_ref) for group in groups}
            for i in range(first, first + 4):
                low, high = (i, mid) if mid // 8 >= i // 8 else (mid, i)
                factor = mat_ref[src, half, pl.ds(low * FLAT + high, 1), :]
                for group in groups:
                    term = factor * rows[group]
                    accs[i, group] = term if mid == 0 else accs[i, group] + term
        for i in range(first, first + 4):
            for group in groups:
                value = accs[i, group]
                start = i * FLAT + 8 * group
                if whole is not None:
                    root = whole[8 * group : 8 * group + 8]
                    value = value * (root / whole[i : i + 1])
                    start = i * PAD + 8 * group
                mat_ref[dst, half, pl.ds(start, 8), :] = value


def tree_order(children_ref, order_ref):
    place = NODES
    parents = [NODES]
    for count in (2, 4, 8, 16, 32):
        place = place - count
        ids = []
        for at, parent in enumerate(parents):
            row = jnp.clip(parent - LEAVES, 0, NODES - LEAVES)
            for side in range(2):
                child = children_ref[side, row]
                order_ref[place + 2 * at + side] = child
                ids.append(child)
        parents = ids


def spread(half, mat_ref, spread_ref):
    for group in range(4):
        block = mat_ref[0, half, group * 120 : group * 120 + LANES, :].T
        for at in range(5):
            i = group * 5 + at
            moved = block if at == 0 else pltpu.roll(block, LANES - PAD * at, 1)
            for k in range(RATES):
                rows = pl.ds(i * RATES + k, SPLIT, stride=SPREAD)
                spread_ref[half, rows, :] = moved[k * SPLIT : (k + 1) * SPLIT]


def parts(half, at, spread_ref):
    value = spread_ref[half, pl.ds(at * SPREAD, ROWS), :]
    value = jnp.where(iota((ROWS, LANES), 1) < STATES, value, 0.0)
    high = value.astype(BF16).astype(F32)
    return high, value - high


def leaf_operands(order_ref, spread_ref, leaf_ref):
    for node in range(LEAVES // 2):
        high, low = parts(0, jnp.clip(order_ref[2 * node], 0, LEAVES - 1), spread_ref)
        leaf_ref[node, 0:ROWS, :] = (high + pltpu.roll(low, 32, 1)).astype(BF16)
        high, low = parts(0, jnp.clip(order_ref[2 * node + 1], 0, LEAVES - 1), spread_ref)
        leaf_ref[node, ROWS : 2 * ROWS, :] = (
            pltpu.roll(high, 64, 1) + pltpu.roll(low, 96, 1)
        ).astype(BF16)


def inner_operands(order_ref, spread_ref, inner_ref):
    row, col = iota((LANES, 256), 0), iota((LANES, 256), 1)
    state = lax.rem(col, ROWS) // RATES
    low_part = (col >= 2 * ROWS).astype(jnp.int32) * 32
    place = jnp.where((row == state + low_part) & (col < 3 * ROWS), 1.0, 0.0).astype(BF16)
    row, col = iota((ROWS, 256), 0), iota((ROWS, 256), 1)
    same = lax.rem(row, RATES) == lax.rem(col, RATES)
    for at in range(INNER):
        child = jnp.clip(order_ref[LEAVES + at] - LEAVES, 0, INNER - 1)
        high, low = parts(1, child, spread_ref)
        both = (high + pltpu.roll(low, 32, 1)).astype(BF16)
        wide = jnp.dot(both, place, preferred_element_type=F32)
        inner_ref[at] = jnp.where(same, wide, 0.0).astype(BF16)


def gather_leaves(chunk, tips_ref, order_ref, flat_ref, leaves_ref):
    tiles = CHUNK // LANES
    for tile in range(tiles):
        lanes = pl.ds(pl.multiple_of(chunk * CHUNK, CHUNK) + tile * LANES, LANES)
        for state in range(STATES):
            rows = pl.ds(state, LEAVES, stride=FLAT)
            flat_ref[tile, rows, :] = tips_ref[state, :, lanes].astype(F32)
    filler = jnp.zeros((SPLIT - PAD, CHUNK), F32)
    for at in range(LEAVES):
        rows = pl.ds(jnp.clip(order_ref[at], 0, LEAVES - 1) * FLAT, PAD)
        value = jnp.concatenate([flat_ref[tile, rows, :] for tile in range(tiles)], axis=1)
        value = jnp.concatenate([value, filler], axis=0).astype(BF16)
        leaves_ref[chunk, at * SPLIT : (at + 1) * SPLIT, :] = value


def keep(ref, chunk, at, value):
    high = value.astype(BF16)
    ref[chunk, at, 0:ROWS, :] = high
    ref[chunk, at, ROWS : 2 * ROWS, :] = (value - high.astype(F32)).astype(BF16)


def prune_leaves(nodes, chunk, leaves_ref, leaf_ref, level_ref):
    for node in nodes:
        left = leaves_ref[chunk, 2 * node * SPLIT : (2 * node + 1) * SPLIT, :]
        right = leaves_ref[chunk, (2 * node + 1) * SPLIT : (2 * node + 2) * SPLIT, :]
        stacked = jnp.concatenate([left, left, right, right], axis=0)
        both = jnp.dot(leaf_ref[node], stacked, preferred_element_type=F32)
        keep(level_ref, chunk, node, both[0:ROWS] * both[ROWS:])


def prune_inner(chunks, inner_ref, level_refs, weight):
    def moved(at, ref, chunk, child):
        high = ref[chunk, child, 0:ROWS, :]
        low = ref[chunk, child, ROWS : 2 * ROWS, :]
        stacked = jnp.concatenate([high, low, high], axis=0)
        return jnp.dot(inner_ref[at, :, 0 : 3 * ROWS], stacked, preferred_element_type=F32)

    scales = [jnp.zeros((1, CHUNK), F32) for _ in range(chunks)]
    results = []
    base = 0
    for level, count in enumerate(LEVEL_NODES):
        ref = level_refs[level]
        parents = count // 2
        for chunk in range(chunks):
            for place in range(parents):
                at = base + 2 * place
                value = moved(at, ref, chunk, 2 * place) * moved(at + 1, ref, chunk, 2 * place + 1)
                if parents == 4:
                    top = jnp.max(value, axis=0, keepdims=True)
                    value = value * (1.0 / top)
                    scales[chunk] = scales[chunk] + jnp.log(top)
                if parents > 1:
                    keep(level_refs[level + 1], chunk, place, value)
                else:
                    lik = jnp.sum(value * weight, axis=0, keepdims=True)
                    results.append(jnp.log(lik) + scales[chunk])
        base = base + count
    return results


def exchange(axis, size, own_ref, buf, send, recv):
    me = lax.axis_index(axis)
    copies = []
    for off in range(1, size):
        copies.append(
            pltpu.make_async_remote_copy(
                src_ref=own_ref,
                dst_ref=buf.at[me],
                send_sem=send.at[off],
                recv_sem=recv.at[off],
                device_id={axis: lax.rem(me + off, size)},
            )
        )
    for copy in copies:
        copy.start()
    buf[me] = own_ref[...]
    return copies


def total_of(copies, buf, size):
    for copy in copies:
        copy.wait()
    summed = buf[0]
    for at in range(1, size):
        summed = summed + buf[at]
    return summed


def kernel(
    mesh_shape,
    children_ref,
    gene_ref,
    count_ref,
    freqs_ref,
    rates_ref,
    branch_ref,
    exchange_ref,
    tips_hbm,
    site_ref,
    sums_ref,
    total_ref,
    tips_ref,
    order_ref,
    leaves_ref,
    pad_ref,
    mat_ref,
    spread_ref,
    leaf_ref,
    inner_ref,
    flat_ref,
    level_refs,
    weight_ref,
    part_ref,
    own_ref,
    site_buf,
    gene_buf,
    fetch_sems,
    site_sems,
    gene_sems,
):
    genes, sites = mesh_shape
    barrier = pltpu.get_barrier_semaphore()
    for axis, size in (("site", sites), ("gene", genes)):
        for off in range(1, size):
            peer = lax.rem(lax.axis_index(axis) + off, size)
            pl.semaphore_signal(barrier, inc=1, device_id={axis: peer})
    chunks = site_ref.shape[1] // CHUNK

    def fetch(chunk):
        lanes = pl.ds(pl.multiple_of(chunk * CHUNK, CHUNK), CHUNK)
        return pltpu.make_async_copy(
            tips_hbm.at[0, :, :, lanes], tips_ref.at[:, :, lanes], fetch_sems.at[chunk]
        )

    for chunk in range(chunks):
        fetch(chunk).start()
    tree_order(children_ref, order_ref)
    for tile in range(CHUNK // LANES):
        flat_ref[tile] = jnp.zeros((LEAVES * FLAT, LANES), F32)
    powers, pi_sub = rate_powers(exchange_ref, freqs_ref, pad_ref)
    for i in range(STATES):
        row = jnp.broadcast_to(pi_sub[i : i + 1, 0:1] / RATES, (RATES, LANES))
        weight_ref[i * RATES : (i + 1) * RATES, :] = row

    taylor(powers, rates_ref, branch_ref, mat_ref)
    per_step = chunks // SQUARINGS

    def gather(step):
        for at in range(per_step):
            chunk = step * per_step + at
            fetch(chunk).wait()
            gather_leaves(chunk, tips_ref, order_ref, flat_ref, leaves_ref)

    def leaf_branches(step, carry):
        gather(step)
        square(step, 0, mat_ref, None)
        return carry

    lax.fori_loop(0, SQUARINGS - 1, leaf_branches, 0)
    gather(SQUARINGS - 1)
    square(SQUARINGS - 1, 0, mat_ref, jnp.sqrt(pi_sub))
    spread(0, mat_ref, spread_ref)
    leaf_operands(order_ref, spread_ref, leaf_ref)

    def inner_branches(step, whole):
        def beside(number):
            for at in range(per_step):
                nodes = range(LEAVES // 2 * number // 5, LEAVES // 2 * (number + 1) // 5)
                prune_leaves(nodes, step * per_step + at, leaves_ref, leaf_ref, level_refs[0])

        square(step, 1, mat_ref, whole, beside)

    def triangles(step, carry):
        inner_branches(step, None)
        return carry

    lax.fori_loop(0, SQUARINGS - 1, triangles, 0)
    inner_branches(SQUARINGS - 1, jnp.sqrt(pi_sub))
    spread(1, mat_ref, spread_ref)
    inner_operands(order_ref, spread_ref, inner_ref)
    results = prune_inner(chunks, inner_ref, level_refs, weight_ref[:, 0:1])
    lane = iota((1, LANES), 1)
    gathered = jnp.zeros((1, LANES), F32)
    for slot in range(chunks * CHUNK // LANES):
        live = count_ref[0, slot]
        gene = gene_ref[0, slot]
        at = slot * LANES % CHUNK
        part = results[slot * LANES // CHUNK][:, at : at + LANES]
        part = jnp.where(lane < live, part, 0.0)
        site_ref[:, slot * LANES : (slot + 1) * LANES] = part
        summed = jnp.sum(part, axis=1, keepdims=True)
        gathered = gathered + jnp.where(lane == gene, summed, 0.0)
        gathered = gathered + jnp.where(lane == gene + GENES, live.astype(F32), 0.0)
    part_ref[...] = gathered
    pl.semaphore_wait(barrier, sites + genes - 2)
    copies = exchange("site", sites, part_ref, site_buf, site_sems.at[0], site_sems.at[1])
    summed = total_of(copies, site_buf, sites)
    own = jnp.sum(jnp.where(lane < GENES, summed, 0.0), axis=1, keepdims=True)
    own_ref[...] = jnp.broadcast_to(own, (1, LANES))
    copies = exchange("gene", genes, own_ref, gene_buf, gene_sems.at[0], gene_sems.at[1])
    sums_ref[...] = summed
    total_ref[...] = total_of(copies, gene_buf, genes)


def likelihoods(genes, width, tips, exchange_, freqs, rates, branch, children, slot_gene, site_count):
    sites = tips.shape[3]
    chunks = sites // CHUNK
    smem = pl.BlockSpec(memory_space=pltpu.SMEM)
    vmem = pl.BlockSpec(memory_space=pltpu.VMEM)
    return pl.pallas_call(
        functools.partial(kernel, (genes, width)),
        name="likelihoods",
        out_shape=(
            jax.ShapeDtypeStruct((1, sites), F32),
            jax.ShapeDtypeStruct((1, LANES), F32),
            jax.ShapeDtypeStruct((1, LANES), F32),
        ),
        in_specs=[smem] * 6 + [vmem, pl.BlockSpec(memory_space=pl.ANY)],
        out_specs=(vmem, vmem, vmem),
        scratch_shapes=[
            pltpu.VMEM((STATES, LEAVES, sites), BF16),
            pltpu.SMEM((NODES,), jnp.int32),
            pltpu.VMEM((chunks, LEAVES * SPLIT, CHUNK), BF16),
            pltpu.VMEM((LANES, LANES), F32),
            pltpu.VMEM((2, 2, 512, LANES), F32),
            pltpu.VMEM((2, SPLIT * SPREAD, LANES), F32),
            pltpu.VMEM((LEAVES // 2, 2 * ROWS, LANES), BF16),
            pltpu.VMEM((INNER, ROWS, 256), BF16),
            pltpu.VMEM((CHUNK // LANES, FLAT * LEAVES, LANES), F32),
            [pltpu.VMEM((chunks, count, 2 * ROWS, CHUNK), BF16) for count in LEVEL_NODES],
            pltpu.VMEM((ROWS, LANES), F32),
            pltpu.VMEM((1, LANES), F32),
            pltpu.VMEM((1, LANES), F32),
            pltpu.VMEM((width, 1, LANES), F32),
            pltpu.VMEM((genes, 1, LANES), F32),
            pltpu.SemaphoreType.DMA((chunks,)),
            pltpu.SemaphoreType.DMA((2, width)),
            pltpu.SemaphoreType.DMA((2, genes)),
        ],
        compiler_params=pltpu.CompilerParams(
            vmem_limit_bytes=60 * 1024 * 1024, collective_id=0, has_side_effects=True
        ),
    )(
        children.T,
        slot_gene,
        site_count,
        freqs,
        rates,
        branch,
        exchange_,
        tips.transpose(0, 2, 1, 3),
    )


def finish_kernel(scale, values_ref, sums_ref, total_ref, site_out, mean_out, total_out):
    site_out[...] = values_ref[...]
    sums = sums_ref[...]
    mean_out[...] = (sums / pltpu.roll(sums, GENES, 1))[:, 0:GENES]
    total_out[...] = total_ref[:, 0:1] * (1.0 / scale)


def finish(values, sums, total, scale):
    vmem = pl.BlockSpec(memory_space=pltpu.VMEM)
    return pl.pallas_call(
        functools.partial(finish_kernel, scale),
        name="finish",
        out_shape=(
            jax.ShapeDtypeStruct(values.shape, F32),
            jax.ShapeDtypeStruct((1, GENES), F32),
            jax.ShapeDtypeStruct((1, 1), F32),
        ),
        in_specs=[vmem] * 3,
        out_specs=(vmem, vmem, vmem),
    )(values, sums, total)


def solution(mesh):
    genes, sites = mesh.shape["gene"], mesh.shape["site"]

    def on_device(*args):
        values, sums, total = likelihoods(genes, sites, *args)
        scale = values.shape[1] * sites
        values, gene_loglik, total = finish(values, sums, total, scale)
        return values, gene_loglik, total.reshape(())

    pair = P("gene", "site")
    return jax.shard_map(
        on_device,
        mesh=mesh,
        in_specs=(P("gene", None, None, "site"), P(), P(), P(), P(), P(), pair, pair),
        out_specs=(pair, P("gene", None), P()),
        check_vma=False,
    )
```

```python
import functools

import jax
import jax.numpy as jnp
from jax import lax
from jax.experimental import pallas as pl
from jax.experimental.pallas import tpu as pltpu
from jax.sharding import PartitionSpec as P

STATES = 20
RATES = 4
ROWS = STATES * RATES
LEAVES = 32
INNER = 30
NODES = 62
GENES = 64
PAD = 24
LANES = 128
SPLIT = 32
CHUNK = 256
LEVEL_NODES = (16, 8, 4, 2)
SQUARINGS = 8
SPREAD = ROWS + 1
FLAT = PAD + 1
F32 = jnp.float32
BF16 = jnp.bfloat16


def iota(shape, axis):
    return lax.broadcasted_iota(jnp.int32, shape, axis)


def rate_powers(exchange_ref, freqs_ref, pad_ref):
    pad_ref[...] = jnp.zeros((LANES, LANES), F32)
    pad_ref[0:STATES, 0:STATES] = exchange_ref[...]
    full = pad_ref[...]
    both = (full + full.T)[0:PAD, :]
    shape = (PAD, LANES)
    sub, lane = iota(shape, 0), iota(shape, 1)
    pi_sub = jnp.zeros(shape, F32)
    pi_lane = jnp.zeros(shape, F32)
    for state in range(STATES):
        value = freqs_ref[state]
        pi_sub = jnp.where(sub == state, value, pi_sub)
        pi_lane = jnp.where(lane == state, value, pi_lane)
    total = jnp.sum(pi_sub, axis=0, keepdims=True)
    pi_sub = pi_sub / total
    pi_lane = pi_lane / total
    sym = jnp.where(sub == lane, 0.0, both * 0.5)
    out_rate = jnp.sum(sym * pi_sub, axis=0, keepdims=True)
    mean_rate = jnp.sum(out_rate * pi_lane[0:1], axis=1, keepdims=True)
    root_sub, root_lane = jnp.sqrt(pi_sub), jnp.sqrt(pi_lane)
    gen = (sym * root_sub * root_lane - jnp.where(sub == lane, out_rate, 0.0)) / mean_rate

    def times(left, right):
        acc = left[:, 0:1] * right[0:1, :]
        for mid in range(1, STATES):
            acc = acc + left[:, mid : mid + 1] * right[mid : mid + 1, :]
        return acc

    second = times(gen, gen) * 0.5
    third = times(second, gen) * (1.0 / 3.0)
    fourth = times(second, second) * (4.0 / 24.0)
    powers = [gen, second, third, fourth]
    for order, part in ((5, gen), (6, second), (7, third), (8, fourth)):
        ratio = {5: 24.0 / 120.0, 6: 48.0 / 720.0, 7: 144.0 / 5040.0, 8: 576.0 / 40320.0}[order]
        powers.append(times(fourth, part) * ratio)
    return powers, pi_sub


def taylor(powers, rates_ref, branch_ref, mat_ref):
    shape = (1, LANES)
    lane = iota(shape, 1)
    category = lane // SPLIT
    rate = jnp.zeros(shape, F32)
    mean = jnp.zeros(shape, F32)
    for k in range(RATES):
        rate = jnp.where(category == k, rates_ref[k], rate)
        mean = mean + rates_ref[k]
    rate = rate / (mean / RATES)
    taus = []
    for half in range(2):
        length = jnp.zeros(shape, F32)
        for at in range(min(SPLIT, NODES - half * SPLIT)):
            length = jnp.where(lane % SPLIT == at, branch_ref[half * SPLIT + at], length)
        taus.append(length * rate / 256.0)
    for i in range(STATES):
        skip = i // 8 * 8
        shape = (PAD - skip, LANES)
        columns = [jnp.broadcast_to(p[skip:, i : i + 1], shape) for p in powers]
        eye = jnp.where(iota(shape, 0) == i - skip, 1.0, 0.0)
        for half in range(2):
            acc = columns[7]
            for order in range(6, -1, -1):
                acc = columns[order] + acc * taus[half]
            acc = eye + acc * taus[half]
            for row in range(0, PAD - skip, 8):
                start = i * FLAT + skip + row
                mat_ref[0, half, pl.ds(start, 8), :] = acc[row : row + 8]


def rows_of(src, half, mid, group, mat_ref):
    if group >= mid // 8:
        return mat_ref[src, half, pl.ds(mid * FLAT + 8 * group, 8), :]
    return mat_ref[src, half, pl.ds(8 * group * FLAT + mid, 8, stride=FLAT), :]


def square(step, half, mat_ref, whole, beside=None):
    src = lax.rem(step, 2)
    dst = 1 - src
    for first in range(0, STATES, 4):
        if beside is not None:
            beside(first // 4)
        groups = range(0 if whole is not None else first // 8, PAD // 8)
        accs = {}
        for mid in range(STATES):
            rows = {group: rows_of(src, half, mid, group, mat_ref) for group in groups}
            for i in range(first, first + 4):
                low, high = (i, mid) if mid // 8 >= i // 8 else (mid, i)
                factor = mat_ref[src, half, pl.ds(low * FLAT + high, 1), :]
                for group in groups:
                    term = factor * rows[group]
                    accs[i, group] = term if mid == 0 else accs[i, group] + term
        for i in range(first, first + 4):
            for group in groups:
                value = accs[i, group]
                start = i * FLAT + 8 * group
                if whole is not None:
                    root, inverse = whole
                    value = value * root[8 * group : 8 * group + 8] * inverse[i : i + 1]
                    start = i * PAD + 8 * group
                mat_ref[dst, half, pl.ds(start, 8), :] = value


def tree_order(children_ref, order_ref):
    place = NODES
    parents = [NODES]
    for count in (2, 4, 8, 16, 32):
        place = place - count
        ids = []
        for at, parent in enumerate(parents):
            row = jnp.clip(parent - LEAVES, 0, NODES - LEAVES)
            for side in range(2):
                child = children_ref[side, row]
                order_ref[place + 2 * at + side] = child
                ids.append(child)
        parents = ids


def spread(half, mat_ref, spread_ref):
    for group in range(4):
        block = mat_ref[0, half, group * 120 : group * 120 + LANES, :].T
        for at in range(5):
            i = group * 5 + at
            moved = block if at == 0 else pltpu.roll(block, LANES - PAD * at, 1)
            for k in range(RATES):
                rows = pl.ds(i * RATES + k, SPLIT, stride=SPREAD)
                spread_ref[half, rows, :] = moved[k * SPLIT : (k + 1) * SPLIT]


def parts(half, at, spread_ref):
    value = spread_ref[half, pl.ds(at * SPREAD, ROWS), :]
    value = jnp.where(iota((ROWS, LANES), 1) < STATES, value, 0.0)
    high = value.astype(BF16).astype(F32)
    return high, value - high


def leaf_operands(order_ref, spread_ref, leaf_ref):
    for node in range(LEAVES // 2):
        high, low = parts(0, jnp.clip(order_ref[2 * node], 0, LEAVES - 1), spread_ref)
        leaf_ref[node, 0:ROWS, :] = (high + pltpu.roll(low, 32, 1)).astype(BF16)
        high, low = parts(0, jnp.clip(order_ref[2 * node + 1], 0, LEAVES - 1), spread_ref)
        leaf_ref[node, ROWS : 2 * ROWS, :] = (
            pltpu.roll(high, 64, 1) + pltpu.roll(low, 96, 1)
        ).astype(BF16)


def inner_operands(order_ref, spread_ref, inner_ref):
    row, col = iota((LANES, 256), 0), iota((LANES, 256), 1)
    state = lax.rem(col, ROWS) // RATES
    low_part = (col >= 2 * ROWS).astype(jnp.int32) * 32
    place = jnp.where((row == state + low_part) & (col < 3 * ROWS), 1.0, 0.0).astype(BF16)
    row, col = iota((ROWS, 256), 0), iota((ROWS, 256), 1)
    same = lax.rem(row, RATES) == lax.rem(col, RATES)
    for at in range(INNER):
        child = jnp.clip(order_ref[LEAVES + at] - LEAVES, 0, INNER - 1)
        high, low = parts(1, child, spread_ref)
        both = (high + pltpu.roll(low, 32, 1)).astype(BF16)
        wide = jnp.dot(both, place, preferred_element_type=F32)
        inner_ref[at] = jnp.where(same, wide, 0.0).astype(BF16)


def gather_leaves(chunk, tips_ref, order_ref, flat_ref, leaves_ref):
    tiles = CHUNK // LANES
    for tile in range(tiles):
        lanes = pl.ds(pl.multiple_of(chunk * CHUNK, CHUNK) + tile * LANES, LANES)
        for state in range(STATES):
            rows = pl.ds(state, LEAVES, stride=FLAT)
            flat_ref[tile, rows, :] = tips_ref[state, :, lanes].astype(F32)
    filler = jnp.zeros((SPLIT - PAD, CHUNK), F32)
    for at in range(LEAVES):
        rows = pl.ds(jnp.clip(order_ref[at], 0, LEAVES - 1) * FLAT, PAD)
        value = jnp.concatenate([flat_ref[tile, rows, :] for tile in range(tiles)], axis=1)
        value = jnp.concatenate([value, filler], axis=0).astype(BF16)
        leaves_ref[chunk, at * SPLIT : (at + 1) * SPLIT, :] = value


def keep(ref, chunk, at, value):
    high = value.astype(BF16)
    ref[chunk, at, 0:ROWS, :] = high
    ref[chunk, at, ROWS : 2 * ROWS, :] = (value - high.astype(F32)).astype(BF16)


def prune_leaves(nodes, chunk, leaves_ref, leaf_ref, level_ref):
    for node in nodes:
        left = leaves_ref[chunk, 2 * node * SPLIT : (2 * node + 1) * SPLIT, :]
        right = leaves_ref[chunk, (2 * node + 1) * SPLIT : (2 * node + 2) * SPLIT, :]
        stacked = jnp.concatenate([left, left, right, right], axis=0)
        both = jnp.dot(leaf_ref[node], stacked, preferred_element_type=F32)
        keep(level_ref, chunk, node, both[0:ROWS] * both[ROWS:])


def prune_inner(chunks, inner_ref, level_refs, weight):
    def moved(at, ref, chunk, child):
        high = ref[chunk, child, 0:ROWS, :]
        low = ref[chunk, child, ROWS : 2 * ROWS, :]
        stacked = jnp.concatenate([high, low, high], axis=0)
        return jnp.dot(inner_ref[at, :, 0 : 3 * ROWS], stacked, preferred_element_type=F32)

    scales = [jnp.zeros((1, CHUNK), F32) for _ in range(chunks)]
    results = []
    base = 0
    for level, count in enumerate(LEVEL_NODES):
        ref = level_refs[level]
        parents = count // 2
        for chunk in range(chunks):
            for place in range(parents):
                at = base + 2 * place
                value = moved(at, ref, chunk, 2 * place) * moved(at + 1, ref, chunk, 2 * place + 1)
                if parents == 4:
                    top = jnp.max(value, axis=0, keepdims=True)
                    value = value * (1.0 / top)
                    scales[chunk] = scales[chunk] + jnp.log(top)
                if parents > 1:
                    keep(level_refs[level + 1], chunk, place, value)
                else:
                    lik = jnp.sum(value * weight, axis=0, keepdims=True)
                    results.append(jnp.log(lik) + scales[chunk])
        base = base + count
    return results


def exchange(axis, size, own_ref, buf, send, recv):
    me = lax.axis_index(axis)
    copies = []
    for off in range(1, size):
        copies.append(
            pltpu.make_async_remote_copy(
                src_ref=own_ref,
                dst_ref=buf.at[me],
                send_sem=send.at[off],
                recv_sem=recv.at[off],
                device_id={axis: lax.rem(me + off, size)},
            )
        )
    for copy in copies:
        copy.start()
    buf[me] = own_ref[...]
    return copies


def total_of(copies, buf, size):
    for copy in copies:
        copy.wait()
    summed = buf[0]
    for at in range(1, size):
        summed = summed + buf[at]
    return summed


def kernel(
    mesh_shape,
    children_ref,
    gene_ref,
    count_ref,
    freqs_ref,
    rates_ref,
    branch_ref,
    exchange_ref,
    tips_hbm,
    site_ref,
    sums_ref,
    total_ref,
    tips_ref,
    order_ref,
    leaves_ref,
    pad_ref,
    mat_ref,
    spread_ref,
    leaf_ref,
    inner_ref,
    flat_ref,
    level_refs,
    weight_ref,
    part_ref,
    own_ref,
    site_buf,
    gene_buf,
    fetch_sems,
    site_sems,
    gene_sems,
):
    genes, sites = mesh_shape
    barrier = pltpu.get_barrier_semaphore()
    chunks = site_ref.shape[1] // CHUNK

    def fetch(chunk):
        lanes = pl.ds(pl.multiple_of(chunk * CHUNK, CHUNK), CHUNK)
        return pltpu.make_async_copy(
            tips_hbm.at[0, :, :, lanes], tips_ref.at[:, :, lanes], fetch_sems.at[chunk]
        )

    for chunk in range(chunks):
        fetch(chunk).start()
    tree_order(children_ref, order_ref)
    for tile in range(CHUNK // LANES):
        flat_ref[tile] = jnp.zeros((LEAVES * FLAT, LANES), F32)
    powers, pi_sub = rate_powers(exchange_ref, freqs_ref, pad_ref)
    for i in range(STATES):
        row = jnp.broadcast_to(pi_sub[i : i + 1, 0:1] / RATES, (RATES, LANES))
        weight_ref[i * RATES : (i + 1) * RATES, :] = row

    taylor(powers, rates_ref, branch_ref, mat_ref)
    per_step = chunks // SQUARINGS

    root = jnp.sqrt(pi_sub)
    whole = (root, 1.0 / root)

    def gather(step):
        for at in range(per_step):
            chunk = step * per_step + at
            fetch(chunk).wait()
            gather_leaves(chunk, tips_ref, order_ref, flat_ref, leaves_ref)

    def leaf_branches(step, carry):
        gather(step)
        square(step, 0, mat_ref, None)
        return carry

    lax.fori_loop(0, SQUARINGS - 1, leaf_branches, 0)
    for axis, size in (("site", sites), ("gene", genes)):
        for off in range(1, size):
            peer = lax.rem(lax.axis_index(axis) + off, size)
            pl.semaphore_signal(barrier, inc=1, device_id={axis: peer})
    gather(SQUARINGS - 1)
    square(SQUARINGS - 1, 0, mat_ref, whole)
    spread(0, mat_ref, spread_ref)
    leaf_operands(order_ref, spread_ref, leaf_ref)

    def inner_branches(step, whole):
        def beside(number):
            for at in range(per_step):
                nodes = range(LEAVES // 2 * number // 5, LEAVES // 2 * (number + 1) // 5)
                prune_leaves(nodes, step * per_step + at, leaves_ref, leaf_ref, level_refs[0])

        square(step, 1, mat_ref, whole, beside)

    def triangles(step, carry):
        inner_branches(step, None)
        return carry

    lax.fori_loop(0, SQUARINGS - 1, triangles, 0)
    inner_branches(SQUARINGS - 1, whole)
    spread(1, mat_ref, spread_ref)
    inner_operands(order_ref, spread_ref, inner_ref)
    results = prune_inner(chunks, inner_ref, level_refs, weight_ref[:, 0:1])
    lane = iota((1, LANES), 1)
    gathered = jnp.zeros((1, LANES), F32)
    for slot in range(chunks * CHUNK // LANES):
        live = count_ref[0, slot]
        gene = gene_ref[0, slot]
        at = slot * LANES % CHUNK
        part = results[slot * LANES // CHUNK][:, at : at + LANES]
        part = jnp.where(lane < live, part, 0.0)
        site_ref[:, slot * LANES : (slot + 1) * LANES] = part
        summed = jnp.sum(part, axis=1, keepdims=True)
        gathered = gathered + jnp.where(lane == gene, summed, 0.0)
        gathered = gathered + jnp.where(lane == gene + GENES, live.astype(F32), 0.0)
    part_ref[...] = gathered
    pl.semaphore_wait(barrier, sites + genes - 2)
    copies = exchange("site", sites, part_ref, site_buf, site_sems.at[0], site_sems.at[1])
    summed = total_of(copies, site_buf, sites)
    own = jnp.sum(jnp.where(lane < GENES, summed, 0.0), axis=1, keepdims=True)
    own_ref[...] = jnp.broadcast_to(own, (1, LANES))
    copies = exchange("gene", genes, own_ref, gene_buf, gene_sems.at[0], gene_sems.at[1])
    sums_ref[...] = summed
    total_ref[...] = total_of(copies, gene_buf, genes)


def likelihoods(genes, width, tips, exchange_, freqs, rates, branch, children, slot_gene, site_count):
    sites = tips.shape[3]
    chunks = sites // CHUNK
    smem = pl.BlockSpec(memory_space=pltpu.SMEM)
    vmem = pl.BlockSpec(memory_space=pltpu.VMEM)
    return pl.pallas_call(
        functools.partial(kernel, (genes, width)),
        name="likelihoods",
        out_shape=(
            jax.ShapeDtypeStruct((1, sites), F32),
            jax.ShapeDtypeStruct((1, LANES), F32),
            jax.ShapeDtypeStruct((1, LANES), F32),
        ),
        in_specs=[smem] * 6 + [vmem, pl.BlockSpec(memory_space=pl.ANY)],
        out_specs=(vmem, vmem, vmem),
        scratch_shapes=[
            pltpu.VMEM((STATES, LEAVES, sites), BF16),
            pltpu.SMEM((NODES,), jnp.int32),
            pltpu.VMEM((chunks, LEAVES * SPLIT, CHUNK), BF16),
            pltpu.VMEM((LANES, LANES), F32),
            pltpu.VMEM((2, 2, 512, LANES), F32),
            pltpu.VMEM((2, SPLIT * SPREAD, LANES), F32),
            pltpu.VMEM((LEAVES // 2, 2 * ROWS, LANES), BF16),
            pltpu.VMEM((INNER, ROWS, 256), BF16),
            pltpu.VMEM((CHUNK // LANES, FLAT * LEAVES, LANES), F32),
            [pltpu.VMEM((chunks, count, 2 * ROWS, CHUNK), BF16) for count in LEVEL_NODES],
            pltpu.VMEM((ROWS, LANES), F32),
            pltpu.VMEM((1, LANES), F32),
            pltpu.VMEM((1, LANES), F32),
            pltpu.VMEM((width, 1, LANES), F32),
            pltpu.VMEM((genes, 1, LANES), F32),
            pltpu.SemaphoreType.DMA((chunks,)),
            pltpu.SemaphoreType.DMA((2, width)),
            pltpu.SemaphoreType.DMA((2, genes)),
        ],
        compiler_params=pltpu.CompilerParams(
            vmem_limit_bytes=60 * 1024 * 1024, collective_id=0, has_side_effects=True
        ),
    )(
        children.T,
        slot_gene,
        site_count,
        freqs,
        rates,
        branch,
        exchange_,
        tips.transpose(0, 2, 1, 3),
    )


def finish_kernel(scale, values_ref, sums_ref, total_ref, site_out, mean_out, total_out):
    site_out[...] = values_ref[...]
    sums = sums_ref[...]
    mean_out[...] = (sums / pltpu.roll(sums, GENES, 1))[:, 0:GENES]
    total_out[...] = total_ref[:, 0:1] * (1.0 / scale)


def finish(values, sums, total, scale):
    vmem = pl.BlockSpec(memory_space=pltpu.VMEM)
    return pl.pallas_call(
        functools.partial(finish_kernel, scale),
        name="finish",
        out_shape=(
            jax.ShapeDtypeStruct(values.shape, F32),
            jax.ShapeDtypeStruct((1, GENES), F32),
            jax.ShapeDtypeStruct((1, 1), F32),
        ),
        in_specs=[vmem] * 3,
        out_specs=(vmem, vmem, vmem),
    )(values, sums, total)


def solution(mesh):
    genes, sites = mesh.shape["gene"], mesh.shape["site"]

    def on_device(*args):
        values, sums, total = likelihoods(genes, sites, *args)
        scale = values.shape[1] * sites
        values, gene_loglik, total = finish(values, sums, total, scale)
        return values, gene_loglik, total.reshape(())

    pair = P("gene", "site")
    return jax.shard_map(
        on_device,
        mesh=mesh,
        in_specs=(P("gene", None, None, "site"), P(), P(), P(), P(), P(), pair, pair),
        out_specs=(pair, P("gene", None), P()),
        check_vma=False,
    )
```
